32 devices in a mesh: seq: 8 (over y, x, core), chan: 4 (over z).
Axes of the slice: x: 2, y: 2, z: 4, core: 2. Of those that a mesh axis runs over, the one named last changes fastest.
Arguments:
- fwd_q: bfloat16 [1024, 4096], P('seq', 'chan'), may hold values from -6 to 6
- fwd_k: bfloat16 [1024, 4096], P('seq', 'chan'), may hold values from -6 to 6
- fwd_v: bfloat16 [1024, 4096], P('seq', 'chan'), may hold values from -6 to 6
- bwd_q: bfloat16 [1024, 4096], P('seq', 'chan'), may hold values from -6 to 6
- bwd_k: bfloat16 [1024, 4096], P('seq', 'chan'), may hold values from -6 to 6
- bwd_v: bfloat16 [1024, 4096], P('seq', 'chan'), may hold values from -6 to 6
- bwd_grad: bfloat16 [1024, 4096], P('seq', 'chan'), may hold values from -6 to 6
- filters: float32 [1024, 1024], P('seq', 'chan'), may hold values from -0.1875 to 0.1875
- skip: float32 [4096], P('chan'), may hold values from -4 to 4
Outputs:
- output: bfloat16 [1024, 4096], P('seq', 'chan')
- grad_query: bfloat16 [1024, 4096], P('seq', 'chan')
- grad_key: bfloat16 [1024, 4096], P('seq', 'chan')
- grad_value: bfloat16 [1024, 4096], P('seq', 'chan')
- grad_filter: float32 [1024, 1024], P('seq', 'chan')
- grad_skip: float32 [4096], P('chan')
The draws below stay inside these ranges and needn't reach their ends.
All inputs are finite; a program needn't handle non-finite values.
Results may differ from the reference program's by a relative error of at most 0.0075.
Values may be sent and summed in bfloat16 or wider, within the bound.
A program may use at most 256 MiB of HBM per device.

```python
import math
import jax
import jax.numpy as jnp
from jax import lax

C = 4096
FILTERS = 1024
SEQ_LEN = 1024


def block_scale(key, shape, shards, smallest, top_value):
    gain, own = 1.0, jax.random.fold_in(key, 6)
    for position, shards_of in shards:
        draws = jnp.exp(jax.random.uniform(jax.random.fold_in(own, position), (shards_of,), jnp.float32, smallest / len(shards), top_value / len(shards)))
        gain = gain * jnp.repeat(draws, shape[position] // shards_of).reshape([-1 if axis == position else 1 for axis in range(len(shape))])
    return gain


def bell_draw(own_key, extent, scale, limit, shards=(), kind=jnp.bfloat16):
    drawn = jax.random.normal(own_key, extent, jnp.float32) * scale
    if len(shards) > 0:
        drawn = block_scale(own_key, extent, shards, -0.22, 0.18) * drawn
    return jnp.clip(drawn, min=-limit, max=limit).astype(kind)


def setup_inputs(seed: int = 0) -> dict:
    streams_of = jax.random.split(jax.random.key(seed), 10)
    fwd_q = bell_draw(streams_of[0], (SEQ_LEN, C), 1.0, 6.0, ((0, 8), (1, 4)))
    fwd_k = bell_draw(streams_of[1], (SEQ_LEN, C), 1.0, 6.0, ((0, 8), (1, 4)))
    fwd_v = bell_draw(streams_of[2], (SEQ_LEN, C), 1.0, 6.0, ((0, 8), (1, 4)))
    bwd_q = bell_draw(streams_of[3], (SEQ_LEN, C), 1.0, 6.0, ((0, 8), (1, 4)))
    bwd_k = bell_draw(streams_of[4], (SEQ_LEN, C), 1.0, 6.0, ((0, 8), (1, 4)))
    bwd_v = bell_draw(streams_of[5], (SEQ_LEN, C), 1.0, 6.0, ((0, 8), (1, 4)))
    bwd_grad = bell_draw(streams_of[6], (SEQ_LEN, C), 1.0, 6.0, ((0, 8), (1, 4)))
    filters = bell_draw(streams_of[7], (SEQ_LEN, FILTERS), SEQ_LEN ** -0.5, 0.1875, ((0, 8), (1, 4)), jnp.float32)
    skip = bell_draw(streams_of[8], (C,), 1.0, 4.0, ((0, 4),), jnp.float32)
    return {"fwd_q": fwd_q, "fwd_k": fwd_k, "fwd_v": fwd_v, "bwd_q": bwd_q, "bwd_k": bwd_k, "bwd_v": bwd_v, "bwd_grad": bwd_grad, "filters": filters, "skip": skip}


def spectrum(values):
    return jnp.fft.rfft(values, n=2 * values.shape[0], axis=0)

def signal(spec, seq_length):
    return jnp.fft.irfft(spec, n=2 * seq_length, axis=0)[:seq_length]

def rounded(values):
    return lax.optimization_barrier(values.astype(jnp.bfloat16)).astype(jnp.float32)

def reference(fwd_q, fwd_k, fwd_v, bwd_q, bwd_k, bwd_v, bwd_grad, filters, skip):
    seq_length, channels = fwd_q.shape
    filter_count = filters.shape[1]
    grad_scale = 1.0 / math.sqrt(seq_length)
    filter_spec = spectrum(filters.astype(jnp.float32))
    out_parts, query_parts, key_parts, value_parts, skip_parts = ([], [], [], [], [])
    filter_total = jnp.zeros((seq_length, filter_count), jnp.float32)
    for group_index in range(channels // filter_count):
        start_col = group_index * filter_count
        stop_col = start_col + filter_count

        def column_block(array):
            return array[:, start_col:stop_col].astype(jnp.float32)
        skip_gain = skip[start_col:stop_col].astype(jnp.float32)
        source = rounded(column_block(fwd_k) * column_block(fwd_v))
        mixed = signal(filter_spec * spectrum(source), seq_length) + skip_gain * source
        out_parts.append((column_block(fwd_q) * mixed).astype(jnp.bfloat16))
        second_source = rounded(column_block(bwd_k) * column_block(bwd_v))
        second_spec = spectrum(second_source)
        mixed_two = signal(filter_spec * second_spec, seq_length) + skip_gain * second_source
        query_parts.append((column_block(bwd_grad) * mixed_two).astype(jnp.bfloat16))
        upstream = rounded(column_block(bwd_grad) * column_block(bwd_q))
        upstream_spec = spectrum(upstream)
        through = signal(jnp.conj(filter_spec) * upstream_spec, seq_length) + skip_gain * upstream
        key_parts.append((through * column_block(bwd_v)).astype(jnp.bfloat16))
        value_parts.append((through * column_block(bwd_k)).astype(jnp.bfloat16))
        filter_total = filter_total + signal(jnp.conj(second_spec) * upstream_spec, seq_length) * grad_scale
        skip_parts.append(lax.optimization_barrier(jnp.sum(upstream * second_source, axis=0)) * grad_scale)
    return (jnp.concatenate(out_parts, axis=1), jnp.concatenate(query_parts, axis=1), jnp.concatenate(key_parts, axis=1), jnp.concatenate(value_parts, axis=1), filter_total, jnp.concatenate(skip_parts, axis=0))
```

```python
import functools
import math

import jax
import jax.numpy as jnp
import numpy as np
from jax import lax
from jax.experimental import pallas as pl
from jax.experimental.pallas import tpu as pltpu
from jax.sharding import PartitionSpec as P

HIGHEST = lax.Precision.HIGHEST
LANES = 128
MESH = pl.DeviceIdType.MESH
BF16 = jnp.bfloat16
F32 = jnp.float32
KERNEL_VMEM = 32 * 2**20


def index_ramp(total):
    return jnp.arange(total, dtype=jnp.int32)


def widened(values):
    return values.astype(jnp.float32)


def angles(out_index, in_index, period, sign):
    phase_steps = out_index[:, None] * in_index[None, :] % period
    phase = phase_steps.astype(jnp.float32) * (sign * 2.0 * math.pi / period)
    return (jnp.cos(phase), jnp.sin(phase))


def times_table(left, right):
    return (left[0] * right[0] - left[1] * right[1], left[0] * right[1] + left[1] * right[0])


def block_table(pair):
    cosine, sine_part = pair
    return jnp.stack([jnp.stack([cosine, -sine_part]), jnp.stack([sine_part, cosine])])


def product_of(left, right):
    return jnp.stack(
        [left[0] * right[0] - left[1] * right[1], left[0] * right[1] + left[1] * right[0]]
    )


def conj_product(left, right):
    return jnp.stack(
        [left[0] * right[0] + left[1] * right[1], left[0] * right[1] - left[1] * right[0]]
    )


def joined(left, right):
    return jnp.concatenate([left, right], axis=-1)


def factor(total):
    chosen = 1
    for candidate in range(1, total + 1):
        if candidate * candidate <= total and total % candidate == 0:
            chosen = candidate
    return chosen


def leading_section(values, seq_size):
    cosine, sine_part = angles(index_ramp(2 * seq_size), index_ramp(seq_size), 2 * seq_size, -1.0)
    table = jnp.stack([cosine, sine_part])
    return jnp.einsum("rkp,pmc->rkmc", table, values, precision=HIGHEST)


def trailing_section(values, seq_size, period):
    cosine, sine_part = angles(index_ramp(seq_size), index_ramp(2 * seq_size), 2 * seq_size, 1.0)
    table = jnp.stack([cosine, -sine_part]) * (1.0 / period)
    return jnp.einsum("rpk,rkmc->pmc", table, values, precision=HIGHEST)


def inner_forward(values, freq_keys, period):
    lead_size, row_count, chan_count = values.shape[1:]
    outer_size = factor(row_count)
    inner_size = row_count // outer_size
    values = values.reshape(2, lead_size, outer_size, inner_size, chan_count)
    first_twiddle = angles(freq_keys, index_ramp(row_count), period, -1.0)
    first_twiddle = tuple(
        (part.reshape(lead_size, outer_size, inner_size) for part in first_twiddle)
    )
    outer_dft = angles(index_ramp(outer_size), index_ramp(outer_size), outer_size, -1.0)
    outer_table = times_table(
        tuple((part[None, :, :, None] for part in outer_dft)),
        tuple((part[:, None, :, :] for part in first_twiddle)),
    )
    values = jnp.einsum("rsjxab,sjabc->rjxbc", block_table(outer_table), values, precision=HIGHEST)
    second_twiddle = angles(index_ramp(outer_size), index_ramp(inner_size), row_count, -1.0)
    inner_dft = angles(index_ramp(inner_size), index_ramp(inner_size), inner_size, -1.0)
    inner_table = times_table(
        tuple((part[None, :, :] for part in inner_dft)),
        tuple((part[:, None, :] for part in second_twiddle)),
    )
    return jnp.einsum("rsxyb,sjxbc->rjxyc", block_table(inner_table), values, precision=HIGHEST)


def inner_inverse(values, freq_keys, period):
    lead_size, outer_size, inner_size, chan_count = values.shape[1:]
    row_count = outer_size * inner_size
    second_twiddle = angles(index_ramp(outer_size), index_ramp(inner_size), row_count, 1.0)
    inner_dft = angles(index_ramp(inner_size), index_ramp(inner_size), inner_size, 1.0)
    inner_table = times_table(
        tuple((part[:, :, None] for part in second_twiddle)),
        tuple((part[None, :, :] for part in inner_dft)),
    )
    values = jnp.einsum("rsxby,sjxyc->rjxbc", block_table(inner_table), values, precision=HIGHEST)
    first_twiddle = angles(freq_keys, index_ramp(row_count), period, 1.0)
    first_twiddle = tuple(
        (part.reshape(lead_size, outer_size, inner_size) for part in first_twiddle)
    )
    outer_dft = angles(index_ramp(outer_size), index_ramp(outer_size), outer_size, 1.0)
    outer_table = times_table(
        tuple((part[:, :, :, None] for part in first_twiddle)),
        tuple((part[None, :, None, :] for part in outer_dft)),
    )
    values = jnp.einsum("rsjabx,sjxbc->rjabc", block_table(outer_table), values, precision=HIGHEST)
    return values.reshape(2, lead_size, row_count, chan_count)


def forward_local(signal_part, seq_size):
    seq_length, chan_count = signal_part.shape
    row_count = seq_length // seq_size
    values = leading_section(signal_part.reshape(seq_size, row_count, chan_count), seq_size)
    return inner_forward(values, index_ramp(2 * seq_size), 2 * seq_length)


def inverse_local(values, seq_size):
    lead_size, outer_size, inner_size, chan_count = values.shape[1:]
    row_count = outer_size * inner_size
    period = 2 * seq_size * row_count
    values = inner_inverse(values, index_ramp(2 * seq_size), period)
    return trailing_section(values, seq_size, period).reshape(seq_size * row_count, chan_count)


def filter_times_pair(spec_filter, spec_pair):
    shape_pair = spec_pair.shape
    width = spec_filter.shape[-1]
    pair_view = spec_pair.reshape(shape_pair[:-1] + (2, width))
    filter_view = spec_filter[..., None, :]
    return product_of(filter_view, pair_view).reshape(shape_pair)


def per_device(fwd_q, fwd_k, fwd_v, bwd_q, bwd_k, bwd_v, bwd_grad, filters, skip):
    row_count, chan_width = fwd_q.shape
    seq_size = lax.axis_size("seq")
    grad_scale = 1.0 / math.sqrt(row_count * seq_size)
    source = (widened(fwd_k) * widened(fwd_v)).astype(jnp.bfloat16)
    second_source = (widened(bwd_k) * widened(bwd_v)).astype(jnp.bfloat16)
    upstream = (widened(bwd_grad) * widened(bwd_q)).astype(jnp.bfloat16)
    skip_gain = widened(skip)
    filters_all = lax.all_gather(filters, "chan", axis=1, tiled=True)
    narrow = chan_width // seq_size
    local_first, local_second = (
        lax.all_to_all(source, "seq", split_axis=1, concat_axis=0, tiled=True),
        lax.all_to_all(second_source, "seq", split_axis=1, concat_axis=0, tiled=True),
    )
    local_filter = lax.all_to_all(filters_all, "seq", split_axis=1, concat_axis=0, tiled=True)
    local_up = lax.all_to_all(upstream, "seq", split_axis=1, concat_axis=0, tiled=True)
    spec_sources = forward_local(
        widened(jnp.concatenate([local_first, local_second], axis=1)), seq_size
    )
    spec_filter = forward_local(local_filter, seq_size)
    conv_local = inverse_local(filter_times_pair(spec_filter, spec_sources), seq_size)
    conv_first, conv_second = (
        lax.all_to_all(conv_local[:, :narrow], "seq", split_axis=0, concat_axis=1, tiled=True),
        lax.all_to_all(conv_local[:, narrow:], "seq", split_axis=0, concat_axis=1, tiled=True),
    )
    spec_up = forward_local(widened(local_up), seq_size)
    spec_second = spec_sources[..., narrow:]
    back_local = inverse_local(
        joined(conj_product(spec_filter, spec_up), conj_product(spec_second, spec_up)), seq_size
    )
    through_conv, filter_terms = (
        lax.all_to_all(back_local[:, :narrow], "seq", split_axis=0, concat_axis=1, tiled=True),
        lax.all_to_all(
            back_local[:, narrow:] * grad_scale, "seq", split_axis=0, concat_axis=1, tiled=True
        ),
    )
    grad_filter = lax.psum_scatter(filter_terms, "chan", scatter_dimension=1, tiled=True)
    source_wide = widened(source)
    second_wide = widened(second_source)
    upstream_wide = widened(upstream)
    mixed = conv_first + skip_gain * source_wide
    output = (widened(fwd_q) * mixed).astype(jnp.bfloat16)
    mixed_two = conv_second + skip_gain * second_wide
    grad_query = (widened(bwd_grad) * mixed_two).astype(jnp.bfloat16)
    through = through_conv + skip_gain * upstream_wide
    grad_key = (through * widened(bwd_v)).astype(jnp.bfloat16)
    grad_value = (through * widened(bwd_k)).astype(jnp.bfloat16)
    grad_skip = lax.psum(jnp.sum(upstream_wide * second_wide, axis=0) * grad_scale, "seq")
    return (output, grad_query, grad_key, grad_value, grad_filter, grad_skip)


def block_tables(rows):
    freq = 2 * np.arange(rows)[:, None] + 1
    phase = (freq * np.arange(rows)[None, :] % (4 * rows)) * (np.pi / (2 * rows))
    forward = np.concatenate([np.cos(phase), -np.sin(phase)], axis=0)
    inverse = np.concatenate([np.cos(phase), -np.sin(phase)], axis=0).T / rows
    return forward.astype(np.float32), inverse.astype(np.float32)


def kernel(
    n, nc, scale,
    fq_h, fk_h, fv_h, bq_h, bk_h, bv_h, bg_h, filt_h, skip_h, fwd_h, inv_h,
    out_o, gq_o, gk_o, gv_o, gf_o, gs_o,
    fq, fk, fv, bq, bk, bv, bg, filt, skip, fwd_t, inv_t, in_sem,
    su_send, s1_send, fz, su, s1, rf, spec_s, spec_u, spec_f, spec_w, prod,
    c_send, c_recv, g_send, rg, zg, k_send, k_recv,
    su_ss, su_rs, s1_ss, s1_rs, f_ss, f_rs, z_ss, z_rs, c_ss, c_rs, g_ss, g_rs, y_ss, y_rs, k_ss, k_rs,
):
    rows, chan_width = fq.shape
    w = chan_width // n
    per = filt.shape[1] // w
    me = lax.axis_index("seq")
    mz = lax.axis_index("chan")
    peers = [lax.rem(me + r, n) for r in range(1, n)]
    senders = peers[::-1]
    zpeers = [lax.rem(mz + r, nc) for r in range(1, nc)]
    started = []

    def lane(p):
        return pl.ds(pl.multiple_of(p * w, w), w)

    def copy(src, dst, ss, rs, to):
        return pltpu.make_async_remote_copy(
            src_ref=src, dst_ref=dst, send_sem=ss, recv_sem=rs, device_id=to, device_id_type=MESH
        )

    def send(src, dst, ss, rs, to):
        c = copy(src, dst, ss, rs, to)
        c.start()
        started.append(c)

    def arrived(buf, ss, rs, to):
        copy(buf, buf, ss, rs, to).wait_recv()

    loads = {}
    order = ((filt_h, filt), (bk_h, bk), (bv_h, bv), (bg_h, bg), (bq_h, bq), (fk_h, fk), (fv_h, fv))
    for at, (far, near) in enumerate(order + ((fwd_h, fwd_t), (inv_h, inv_t), (skip_h, skip), (fq_h, fq))):
        loads[id(near)] = pltpu.make_async_copy(far, near, in_sem.at[at])
        loads[id(near)].start()

    def loaded(*refs):
        for ref in refs:
            loads[id(ref)].wait()

    barrier = pltpu.get_barrier_semaphore()
    for p in peers:
        pl.semaphore_signal(barrier, inc=1, device_id={"seq": p}, device_id_type=MESH)
    for z in zpeers:
        pl.semaphore_signal(barrier, inc=1, device_id={"chan": z}, device_id_type=MESH)

    def transform(dst, q, block):
        dst[q] = jnp.dot(fwd_t[...], block, preferred_element_type=F32)

    def gate_block(p):
        at = lane(p)
        su_send[p, 0] = (bk[:, at].astype(F32) * bv[:, at].astype(F32)).astype(BF16)
        su_send[p, 1] = (bg[:, at].astype(F32) * bq[:, at].astype(F32)).astype(BF16)

    loaded(filt)
    for h in range(per):
        fz[mz * per + h] = filt[:, h * w:(h + 1) * w].astype(BF16)
    pl.semaphore_wait(barrier, n - 1 + nc - 1)
    for z in zpeers:
        part = fz.at[pl.ds(mz * per, per)]
        send(part, part, z_ss.at[z], z_rs.at[mz], {"chan": z})
    loaded(bk, bv, bg, bq)
    for p in peers:
        gate_block(p)
        send(su_send.at[p], su.at[me], su_ss.at[p], su_rs.at[me], {"seq": p})
    gate_block(me)
    su[me] = su_send[me]
    loaded(fk, fv)
    for p in range(n):
        cols = slice(p * w, (p + 1) * w)
        s1_send[p] = (fk[:, cols].astype(F32) * fv[:, cols].astype(F32)).astype(BF16)
    s1[me] = s1_send[me]
    loaded(fwd_t, inv_t)
    transform(spec_s, me, su[me, 0])
    transform(spec_u, me, su[me, 1])
    for z in zpeers:
        arrived(fz.at[pl.ds(z * per, per)], z_ss.at[z], z_rs.at[z], {"chan": z})
    for p in peers:
        send(fz.at[p], rf.at[me], f_ss.at[p], f_rs.at[me], {"seq": p})
    for p in peers:
        send(s1_send.at[p], s1.at[me], s1_ss.at[p], s1_rs.at[me], {"seq": p})
    rf[me] = fz[me]

    sign = 1.0 - 2.0 * lax.rem(lax.broadcasted_iota(jnp.int32, (rows, w), 0), 2).astype(F32)

    def windowed(src):
        spec_w[0] = src[0]
        for d in range(1, n):
            spec_w[d, :rows] = src[d, :rows] - sign * src[d - 1, rows:]
            spec_w[d, rows:] = src[d, rows:] + sign * src[d - 1, :rows]

    def products(src, corr):
        def tile(k, carry):
            re_at = pl.ds(pl.multiple_of(k * 8, 8), 8)
            im_at = pl.ds(pl.multiple_of(rows + k * 8, 8), 8)
            ar = [spec_w[d, re_at] for d in range(n)]
            ai = [spec_w[d, im_at] for d in range(n)]
            xr = [src[d, re_at] for d in range(n)]
            xi = [src[d, im_at] for d in range(n)]
            for b in range(n):
                terms = [(c - b, c) for c in range(b, n)] if corr else [(b - c, c) for c in range(b + 1)]
                re, im = None, None
                for d, c in terms:
                    if corr:
                        tr = ar[d] * xr[c] + ai[d] * xi[c]
                        ti = ar[d] * xi[c] - ai[d] * xr[c]
                    else:
                        tr = ar[d] * xr[c] - ai[d] * xi[c]
                        ti = ar[d] * xi[c] + ai[d] * xr[c]
                    re = tr if re is None else re + tr
                    im = ti if im is None else im + ti
                prod[b, re_at] = re
                prod[b, im_at] = im
            return carry

        lax.fori_loop(0, rows // 8, tile, 0)

    def inverse(b):
        return jnp.dot(inv_t[...], prod[b].astype(BF16), preferred_element_type=F32)

    def give_back(which):
        for p in peers:
            c_send[which, p] = inverse(p).astype(BF16)
            send(c_send.at[which, p], c_recv.at[which, me], c_ss.at[which, p], c_rs.at[which, me], {"seq": p})
        c_recv[which, me] = inverse(me).astype(BF16)

    total = jnp.zeros((1, w), F32)
    for q in [me] + senders:
        if q is not me:
            arrived(su.at[q], su_ss.at[q], su_rs.at[q], {"seq": q})
            transform(spec_s, q, su[q, 0])
            transform(spec_u, q, su[q, 1])
        total += jnp.sum(su[q, 0].astype(F32) * su[q, 1].astype(F32), axis=0, keepdims=True)
    k_send[...] = jnp.broadcast_to(total * scale, k_send.shape)
    for p in peers:
        send(k_send, k_recv.at[me], k_ss.at[p], k_rs.at[me], {"seq": p})
    k_recv[me] = k_send[...]

    windowed(spec_s)
    products(spec_u, True)
    for p in peers:
        g_send[p] = (inverse(p) * scale).astype(BF16)
        send(g_send.at[p], rg.at[me], g_ss.at[p], g_rs.at[me], {"seq": p})
    rg[me] = (inverse(me) * scale).astype(BF16)

    for q in [me] + senders:
        if q is not me:
            arrived(rf.at[q], f_ss.at[q], f_rs.at[q], {"seq": q})
        transform(spec_f, q, rf[q])
    windowed(spec_f)
    products(spec_s, False)
    give_back(0)
    products(spec_u, True)
    give_back(1)

    for q in [me] + senders:
        if q is not me:
            arrived(s1.at[q], s1_ss.at[q], s1_rs.at[q], {"seq": q})
        transform(spec_s, q, s1[q])
    products(spec_s, False)
    give_back(2)

    for q in senders:
        arrived(rg.at[q], g_ss.at[q], g_rs.at[q], {"seq": q})
    for z in zpeers:
        send(rg.at[pl.ds(z * per, per)], zg.at[mz], y_ss.at[z], y_rs.at[mz], {"chan": z})

    loaded(skip, fq)
    for q in [me] + senders:
        at = lane(q)
        gain = skip[:, at]
        if q is not me:
            arrived(c_recv.at[0, q], c_ss.at[0, q], c_rs.at[0, q], {"seq": q})
        mixed = c_recv[0, q].astype(F32) + gain * su_send[q, 0].astype(F32)
        gq_o[:, at] = (bg[:, at].astype(F32) * mixed).astype(BF16)
    for q in [me] + senders:
        at = lane(q)
        gain = skip[:, at]
        if q is not me:
            arrived(c_recv.at[1, q], c_ss.at[1, q], c_rs.at[1, q], {"seq": q})
        through = c_recv[1, q].astype(F32) + gain * su_send[q, 1].astype(F32)
        gk_o[:, at] = (through * bv[:, at].astype(F32)).astype(BF16)
        gv_o[:, at] = (through * bk[:, at].astype(F32)).astype(BF16)
    for z in zpeers:
        arrived(zg.at[z], y_ss.at[z], y_rs.at[z], {"chan": z})
    for h in range(per):
        acc = rg[mz * per + h].astype(F32)
        for z in zpeers:
            acc += zg[z, h].astype(F32)
        gf_o[:, h * w:(h + 1) * w] = acc
    for q in senders:
        arrived(k_recv.at[q], k_ss.at[q], k_rs.at[q], {"seq": q})
    for q in range(n):
        gs_o[:, q * w:(q + 1) * w] = k_recv[q, 0:1]
    for q in [me] + senders:
        at = lane(q)
        gain = skip[:, at]
        if q is not me:
            arrived(c_recv.at[2, q], c_ss.at[2, q], c_rs.at[2, q], {"seq": q})
        mixed = c_recv[2, q].astype(F32) + gain * s1_send[q].astype(F32)
        out_o[:, at] = (fq[:, at].astype(F32) * mixed).astype(BF16)
    for c in started:
        c.wait_send()


def store_all(*refs):
    count = len(refs) // 2
    near, far, sems = refs[:count], refs[count:2 * count], refs[-1]
    stores = [pltpu.make_async_copy(near[i], far[i], sems.at[i]) for i in range(count)]
    for c in stores:
        c.start()
    for c in stores:
        c.wait()


def fused_device(n, nc, *args):
    fwd_q, filters, skip = args[0], args[7], args[8]
    rows, chan_width = fwd_q.shape
    w = chan_width // n
    per = filters.shape[1] // w
    scale = 1.0 / math.sqrt(rows * n)
    forward, inverse = (jnp.asarray(t, dtype=BF16) for t in block_tables(rows))
    results = (
        *[pltpu.VMEM((rows, chan_width), BF16)] * 4, pltpu.VMEM(filters.shape, F32), pltpu.VMEM((1, chan_width), F32),
    )
    dma = pltpu.SemaphoreType.DMA
    block = (n, rows, w)
    spectrum = (n, 2 * rows, w)
    scratch = [
        *[pltpu.VMEM((rows, chan_width), BF16)] * 7, pltpu.VMEM(filters.shape, F32),
        pltpu.VMEM((1, chan_width), F32), pltpu.VMEM(forward.shape, BF16), pltpu.VMEM(inverse.shape, BF16),
        dma((11,)),
        pltpu.VMEM((n, 2, rows, w), BF16), pltpu.VMEM(block, BF16), pltpu.VMEM(block, BF16),
        pltpu.VMEM((n, 2, rows, w), BF16), pltpu.VMEM(block, BF16), pltpu.VMEM(block, BF16),
        *[pltpu.VMEM(spectrum, F32)] * 5,
        pltpu.VMEM((3,) + block, BF16), pltpu.VMEM((3,) + block, BF16),
        pltpu.VMEM(block, BF16), pltpu.VMEM(block, BF16), pltpu.VMEM((nc, per, rows, w), BF16),
        pltpu.VMEM((8, w), F32), pltpu.VMEM((n, 8, w), F32),
        dma((n,)), dma((n,)), dma((n,)), dma((n,)), dma((n,)), dma((n,)), dma((nc,)), dma((nc,)),
        dma((3, n)), dma((3, n)), dma((n,)), dma((n,)), dma((nc,)), dma((nc,)), dma((n,)), dma((n,)),
    ]
    operands = (*args[:8], skip.reshape(1, chan_width), forward, inverse)
    hbm, vmem = (pl.BlockSpec(memory_space=m) for m in (pltpu.HBM, pltpu.VMEM))
    outs = pl.pallas_call(
        functools.partial(kernel, n, nc, scale),
        out_shape=results,
        in_specs=[hbm] * 11,
        out_specs=(vmem,) * 6,
        scratch_shapes=scratch,
        compiler_params=pltpu.CompilerParams(
            collective_id=0, has_side_effects=True, vmem_limit_bytes=KERNEL_VMEM
        ),
    )(*[pltpu.with_memory_space_constraint(a, pltpu.HBM) for a in operands])
    outs = pl.pallas_call(
        store_all,
        out_shape=tuple(jax.ShapeDtypeStruct(o.shape, o.dtype) for o in outs),
        in_specs=[vmem] * 6,
        out_specs=(hbm,) * 6,
        scratch_shapes=[dma((6,))],
        compiler_params=pltpu.CompilerParams(vmem_limit_bytes=KERNEL_VMEM),
    )(*outs)
    return tuple(outs[:5]) + (outs[5].reshape(chan_width),)


def routed(*args):
    n, nc = lax.axis_size("seq"), lax.axis_size("chan")
    rows, chan_width = args[0].shape
    filter_width = args[7].shape[1]
    fits = chan_width % (n * LANES) == 0 and rows % 16 == 0
    if fits and filter_width * nc == chan_width and filter_width % (chan_width // n) == 0:
        return fused_device(n, nc, *args)
    return per_device(*args)


def solution(mesh):
    return jax.shard_map(
        routed,
        mesh=mesh,
        in_specs=(
            P("seq", "chan"),
            P("seq", "chan"),
            P("seq", "chan"),
            P("seq", "chan"),
            P("seq", "chan"),
            P("seq", "chan"),
            P("seq", "chan"),
            P("seq", "chan"),
            P("chan"),
        ),
        out_specs=(
            P("seq", "chan"),
            P("seq", "chan"),
            P("seq", "chan"),
            P("seq", "chan"),
            P("seq", "chan"),
            P("chan"),
        ),
        check_vma=False,
    )
```

```python
import functools
import math

import jax
import jax.numpy as jnp
import numpy as np
from jax import lax
from jax.experimental import pallas as pl
from jax.experimental.pallas import tpu as pltpu
from jax.sharding import PartitionSpec as P

HIGHEST = lax.Precision.HIGHEST
LANES = 128
MESH = pl.DeviceIdType.MESH
BF16 = jnp.bfloat16
F32 = jnp.float32
KERNEL_VMEM = 32 * 2**20


def index_ramp(total):
    return jnp.arange(total, dtype=jnp.int32)


def widened(values):
    return values.astype(jnp.float32)


def angles(out_index, in_index, period, sign):
    phase_steps = out_index[:, None] * in_index[None, :] % period
    phase = phase_steps.astype(jnp.float32) * (sign * 2.0 * math.pi / period)
    return (jnp.cos(phase), jnp.sin(phase))


def times_table(left, right):
    return (left[0] * right[0] - left[1] * right[1], left[0] * right[1] + left[1] * right[0])


def block_table(pair):
    cosine, sine_part = pair
    return jnp.stack([jnp.stack([cosine, -sine_part]), jnp.stack([sine_part, cosine])])


def product_of(left, right):
    return jnp.stack(
        [left[0] * right[0] - left[1] * right[1], left[0] * right[1] + left[1] * right[0]]
    )


def conj_product(left, right):
    return jnp.stack(
        [left[0] * right[0] + left[1] * right[1], left[0] * right[1] - left[1] * right[0]]
    )


def joined(left, right):
    return jnp.concatenate([left, right], axis=-1)


def factor(total):
    chosen = 1
    for candidate in range(1, total + 1):
        if candidate * candidate <= total and total % candidate == 0:
            chosen = candidate
    return chosen


def leading_section(values, seq_size):
    cosine, sine_part = angles(index_ramp(2 * seq_size), index_ramp(seq_size), 2 * seq_size, -1.0)
    table = jnp.stack([cosine, sine_part])
    return jnp.einsum("rkp,pmc->rkmc", table, values, precision=HIGHEST)


def trailing_section(values, seq_size, period):
    cosine, sine_part = angles(index_ramp(seq_size), index_ramp(2 * seq_size), 2 * seq_size, 1.0)
    table = jnp.stack([cosine, -sine_part]) * (1.0 / period)
    return jnp.einsum("rpk,rkmc->pmc", table, values, precision=HIGHEST)


def inner_forward(values, freq_keys, period):
    lead_size, row_count, chan_count = values.shape[1:]
    outer_size = factor(row_count)
    inner_size = row_count // outer_size
    values = values.reshape(2, lead_size, outer_size, inner_size, chan_count)
    first_twiddle = angles(freq_keys, index_ramp(row_count), period, -1.0)
    first_twiddle = tuple(
        (part.reshape(lead_size, outer_size, inner_size) for part in first_twiddle)
    )
    outer_dft = angles(index_ramp(outer_size), index_ramp(outer_size), outer_size, -1.0)
    outer_table = times_table(
        tuple((part[None, :, :, None] for part in outer_dft)),
        tuple((part[:, None, :, :] for part in first_twiddle)),
    )
    values = jnp.einsum("rsjxab,sjabc->rjxbc", block_table(outer_table), values, precision=HIGHEST)
    second_twiddle = angles(index_ramp(outer_size), index_ramp(inner_size), row_count, -1.0)
    inner_dft = angles(index_ramp(inner_size), index_ramp(inner_size), inner_size, -1.0)
    inner_table = times_table(
        tuple((part[None, :, :] for part in inner_dft)),
        tuple((part[:, None, :] for part in second_twiddle)),
    )
    return jnp.einsum("rsxyb,sjxbc->rjxyc", block_table(inner_table), values, precision=HIGHEST)


def inner_inverse(values, freq_keys, period):
    lead_size, outer_size, inner_size, chan_count = values.shape[1:]
    row_count = outer_size * inner_size
    second_twiddle = angles(index_ramp(outer_size), index_ramp(inner_size), row_count, 1.0)
    inner_dft = angles(index_ramp(inner_size), index_ramp(inner_size), inner_size, 1.0)
    inner_table = times_table(
        tuple((part[:, :, None] for part in second_twiddle)),
        tuple((part[None, :, :] for part in inner_dft)),
    )
    values = jnp.einsum("rsxby,sjxyc->rjxbc", block_table(inner_table), values, precision=HIGHEST)
    first_twiddle = angles(freq_keys, index_ramp(row_count), period, 1.0)
    first_twiddle = tuple(
        (part.reshape(lead_size, outer_size, inner_size) for part in first_twiddle)
    )
    outer_dft = angles(index_ramp(outer_size), index_ramp(outer_size), outer_size, 1.0)
    outer_table = times_table(
        tuple((part[:, :, :, None] for part in first_twiddle)),
        tuple((part[None, :, None, :] for part in outer_dft)),
    )
    values = jnp.einsum("rsjabx,sjxbc->rjabc", block_table(outer_table), values, precision=HIGHEST)
    return values.reshape(2, lead_size, row_count, chan_count)


def forward_local(signal_part, seq_size):
    seq_length, chan_count = signal_part.shape
    row_count = seq_length // seq_size
    values = leading_section(signal_part.reshape(seq_size, row_count, chan_count), seq_size)
    return inner_forward(values, index_ramp(2 * seq_size), 2 * seq_length)


def inverse_local(values, seq_size):
    lead_size, outer_size, inner_size, chan_count = values.shape[1:]
    row_count = outer_size * inner_size
    period = 2 * seq_size * row_count
    values = inner_inverse(values, index_ramp(2 * seq_size), period)
    return trailing_section(values, seq_size, period).reshape(seq_size * row_count, chan_count)


def filter_times_pair(spec_filter, spec_pair):
    shape_pair = spec_pair.shape
    width = spec_filter.shape[-1]
    pair_view = spec_pair.reshape(shape_pair[:-1] + (2, width))
    filter_view = spec_filter[..., None, :]
    return product_of(filter_view, pair_view).reshape(shape_pair)


def per_device(fwd_q, fwd_k, fwd_v, bwd_q, bwd_k, bwd_v, bwd_grad, filters, skip):
    row_count, chan_width = fwd_q.shape
    seq_size = lax.axis_size("seq")
    grad_scale = 1.0 / math.sqrt(row_count * seq_size)
    source = (widened(fwd_k) * widened(fwd_v)).astype(jnp.bfloat16)
    second_source = (widened(bwd_k) * widened(bwd_v)).astype(jnp.bfloat16)
    upstream = (widened(bwd_grad) * widened(bwd_q)).astype(jnp.bfloat16)
    skip_gain = widened(skip)
    filters_all = lax.all_gather(filters, "chan", axis=1, tiled=True)
    narrow = chan_width // seq_size
    local_first, local_second = (
        lax.all_to_all(source, "seq", split_axis=1, concat_axis=0, tiled=True),
        lax.all_to_all(second_source, "seq", split_axis=1, concat_axis=0, tiled=True),
    )
    local_filter = lax.all_to_all(filters_all, "seq", split_axis=1, concat_axis=0, tiled=True)
    local_up = lax.all_to_all(upstream, "seq", split_axis=1, concat_axis=0, tiled=True)
    spec_sources = forward_local(
        widened(jnp.concatenate([local_first, local_second], axis=1)), seq_size
    )
    spec_filter = forward_local(local_filter, seq_size)
    conv_local = inverse_local(filter_times_pair(spec_filter, spec_sources), seq_size)
    conv_first, conv_second = (
        lax.all_to_all(conv_local[:, :narrow], "seq", split_axis=0, concat_axis=1, tiled=True),
        lax.all_to_all(conv_local[:, narrow:], "seq", split_axis=0, concat_axis=1, tiled=True),
    )
    spec_up = forward_local(widened(local_up), seq_size)
    spec_second = spec_sources[..., narrow:]
    back_local = inverse_local(
        joined(conj_product(spec_filter, spec_up), conj_product(spec_second, spec_up)), seq_size
    )
    through_conv, filter_terms = (
        lax.all_to_all(back_local[:, :narrow], "seq", split_axis=0, concat_axis=1, tiled=True),
        lax.all_to_all(
            back_local[:, narrow:] * grad_scale, "seq", split_axis=0, concat_axis=1, tiled=True
        ),
    )
    grad_filter = lax.psum_scatter(filter_terms, "chan", scatter_dimension=1, tiled=True)
    source_wide = widened(source)
    second_wide = widened(second_source)
    upstream_wide = widened(upstream)
    mixed = conv_first + skip_gain * source_wide
    output = (widened(fwd_q) * mixed).astype(jnp.bfloat16)
    mixed_two = conv_second + skip_gain * second_wide
    grad_query = (widened(bwd_grad) * mixed_two).astype(jnp.bfloat16)
    through = through_conv + skip_gain * upstream_wide
    grad_key = (through * widened(bwd_v)).astype(jnp.bfloat16)
    grad_value = (through * widened(bwd_k)).astype(jnp.bfloat16)
    grad_skip = lax.psum(jnp.sum(upstream_wide * second_wide, axis=0) * grad_scale, "seq")
    return (output, grad_query, grad_key, grad_value, grad_filter, grad_skip)


def block_tables(rows):
    freq = 2 * np.arange(rows)[:, None] + 1
    phase = (freq * np.arange(rows)[None, :] % (4 * rows)) * (np.pi / (2 * rows))
    forward = np.concatenate([np.cos(phase), -np.sin(phase)], axis=0)
    inverse = np.concatenate([np.cos(phase), -np.sin(phase)], axis=0).T / rows
    return forward.astype(np.float32), inverse.astype(np.float32)


REACH = 2


def kernel(
    n, nc, scale,
    fq_h, fk_h, fv_h, bq_h, bk_h, bv_h, bg_h, filt_h, skip_h, fwd_h, inv_h,
    out_o, gq_o, gk_o, gv_o, gf_o, gs_o,
    fq, fk, fv, bq, bk, bv, bg, filt, skip, fwd_t, inv_t, in_sem,
    su_send, s1_send, fz, su, s1, rf, spec_s, spec_u, spec_f, spec_w, prod,
    c_send, c_recv, g_send, zg, g2_send, g2_recv, g3, k_send, k_recv,
    su_ss, su_rs, s1_ss, s1_rs, f_ss, f_rs, z_ss, z_rs, y_ss, c_ss, c_rs,
    gz_ss, gz_rs, g2_ss, g2_rs, g3_ss, g3_rs, k_ss, k_rs,
):
    rows, chan_width = fq.shape
    w = chan_width // n
    per = filt.shape[1] // w
    part, half = rows // nc, rows // 2
    me = lax.axis_index("seq")
    mz = lax.axis_index("chan")

    def flipped(r):
        at, bit = me, 1
        while bit < n:
            if r & bit:
                at = at + bit * (1 - 2 * lax.rem(me // bit, 2))
            bit *= 2
        return at

    order = sorted(range(1, n), key=lambda r: (r < 2, r & 1, -r))
    peers = [flipped(r) for r in order]
    upward = 2 * mz < nc
    zorder = []
    for k in range(nc - 1):
        j = nc - 1 - k
        zorder.append(jnp.where(upward, jnp.where(mz <= k, k + 1, k), jnp.where(mz >= j, j - 1, j)))

    def near(z):
        return (z - mz <= REACH) & (mz - z <= REACH)

    def lane(p):
        return pl.ds(pl.multiple_of(p * w, w), w)

    def copy(src, dst, ss, rs, to):
        return pltpu.make_async_remote_copy(
            src_ref=src, dst_ref=dst, send_sem=ss, recv_sem=rs, device_id=to, device_id_type=MESH
        )

    started = []

    def send(src, dst, ss, rs, to):
        c = copy(src, dst, ss, rs, to)
        c.start()
        started.append(c)

    def arrived(buf, ss, rs, to):
        copy(buf, buf, ss, rs, to).wait_recv()

    loads = {}
    order_in = ((filt_h, filt), (bk_h, bk), (bv_h, bv), (bg_h, bg), (bq_h, bq), (fk_h, fk), (fv_h, fv))
    for at, (far, dst) in enumerate(order_in + ((fwd_h, fwd_t), (inv_h, inv_t), (skip_h, skip), (fq_h, fq))):
        loads[id(dst)] = pltpu.make_async_copy(far, dst, in_sem.at[at])
        loads[id(dst)].start()

    def loaded(*refs):
        for ref in refs:
            loads[id(ref)].wait()

    barrier = pltpu.get_barrier_semaphore()
    for p in peers:
        pl.semaphore_signal(barrier, inc=1, device_id={"seq": p}, device_id_type=MESH)
    greeted = n - 1
    for z in zorder:
        greeted = greeted + near(z).astype(jnp.int32)

        @pl.when(near(z))
        def _(z=z):
            pl.semaphore_signal(barrier, inc=1, device_id={"chan": z}, device_id_type=MESH)

    def transform(dst, q, block):
        dst[q] = jnp.dot(fwd_t[...], block, preferred_element_type=F32)

    loaded(filt)
    for h in range(per):
        fz[mz * per + h] = filt[:, h * w:(h + 1) * w].astype(BF16)
    loaded(bk, bv, bg, bq)
    for p in range(n):
        cols = slice(p * w, (p + 1) * w)
        su_send[p, 0] = (bk[:, cols].astype(F32) * bv[:, cols].astype(F32)).astype(BF16)
        su_send[p, 1] = (bg[:, cols].astype(F32) * bq[:, cols].astype(F32)).astype(BF16)
    pl.semaphore_wait(barrier, greeted)

    def chan_copy(k, h):
        block = fz.at[mz * per + h]
        return copy(block, block, z_ss.at[k, h], z_rs.at[mz, h], {"chan": zorder[k]})

    def relay_copy(o, h, to):
        block = fz.at[o * per + h]
        return copy(block, block, y_ss.at[h], z_rs.at[o, h], {"chan": to})

    def forward(o, h):
        p = o * per + h

        @pl.when(p != me)
        def _():
            copy(fz.at[p], rf.at[me], f_ss.at[p], f_rs.at[me], {"seq": p}).start()

    for k in range(nc - 2, -1, -1):
        @pl.when(near(zorder[k]))
        def _(k=k):
            for h in range(per):
                chan_copy(k, h).start()
    for h in range(per):
        forward(mz, h)
    for p in peers:
        send(su_send.at[p], su.at[me], su_ss.at[p], su_rs.at[me], {"seq": p})

    loaded(fk, fv)
    for p in range(n):
        cols = slice(p * w, (p + 1) * w)
        s1_send[p] = (fk[:, cols].astype(F32) * fv[:, cols].astype(F32)).astype(BF16)
    su[me] = su_send[me]
    s1[me] = s1_send[me]
    loaded(fwd_t, inv_t)
    transform(spec_s, me, su[me, 0])
    transform(spec_u, me, su[me, 1])

    def send_s1(j):
        piece = pl.ds(j * half, half)
        for p in peers:
            send(s1_send.at[p, piece], s1.at[me, piece], s1_ss.at[p, j], s1_rs.at[me, j], {"seq": p})

    relays = []
    for k in range(nc - 1):
        o = zorder[k]
        if k == nc - 2:
            send_s1(0)
            to = jnp.where(o > mz, mz - 1, mz + 1)
            far = jnp.where(o > mz, o - mz, mz - o)
            relays.append(((far == REACH) & (to >= 0) & (to < nc), o, to))
        for h in range(per):
            arrived(fz.at[o * per + h], z_ss.at[k, h], z_rs.at[o, h], {"chan": o})
            for on, origin, to in relays:
                @pl.when(on)
                def _(origin=origin, to=to, h=h):
                    relay_copy(origin, h, to).start()
            forward(o, h)
    rf[me] = fz[me]
    if nc == 1:
        send_s1(0)
    send_s1(1)

    sign = 1.0 - 2.0 * lax.rem(lax.broadcasted_iota(jnp.int32, (rows, w), 0), 2).astype(F32)

    def windowed(src):
        spec_w[0] = src[0]
        for d in range(1, n):
            spec_w[d, :rows] = src[d, :rows] - sign * src[d - 1, rows:]
            spec_w[d, rows:] = src[d, rows:] + sign * src[d - 1, :rows]

    def products(src, corr):
        def tile(k, carry):
            re_at = pl.ds(pl.multiple_of(k * 8, 8), 8)
            im_at = pl.ds(pl.multiple_of(rows + k * 8, 8), 8)
            ar = [spec_w[d, re_at] for d in range(n)]
            ai = [spec_w[d, im_at] for d in range(n)]
            xr = [src[d, re_at] for d in range(n)]
            xi = [src[d, im_at] for d in range(n)]
            for b in range(n):
                terms = [(c - b, c) for c in range(b, n)] if corr else [(b - c, c) for c in range(b + 1)]
                re, im = None, None
                for d, c in terms:
                    if corr:
                        tr = ar[d] * xr[c] + ai[d] * xi[c]
                        ti = ar[d] * xi[c] - ai[d] * xr[c]
                    else:
                        tr = ar[d] * xr[c] - ai[d] * xi[c]
                        ti = ar[d] * xi[c] + ai[d] * xr[c]
                    re = tr if re is None else re + tr
                    im = ti if im is None else im + ti
                prod[b, re_at] = re
                prod[b, im_at] = im
            return carry

        lax.fori_loop(0, rows // 8, tile, 0)

    def inverse(b):
        return jnp.dot(inv_t[...], prod[b].astype(BF16), preferred_element_type=F32)

    def give_back(which):
        for p in peers:
            send(c_send.at[which, p], c_recv.at[which, me], c_ss.at[which, p], c_rs.at[which, me], {"seq": p})

    def outputs(which, now):
        for p in peers:
            c_send[which, p] = inverse(p).astype(BF16)
            if now:
                send(c_send.at[which, p], c_recv.at[which, me], c_ss.at[which, p], c_rs.at[which, me], {"seq": p})
        c_recv[which, me] = inverse(me).astype(BF16)

    total = jnp.zeros((1, w), F32)
    for q in [me] + peers:
        if q is not me:
            arrived(su.at[q], su_ss.at[q], su_rs.at[q], {"seq": q})
            transform(spec_s, q, su[q, 0])
            transform(spec_u, q, su[q, 1])
        total += jnp.sum(su[q, 0].astype(F32) * su[q, 1].astype(F32), axis=0, keepdims=True)
    k_send[...] = jnp.broadcast_to(total * scale, k_send.shape)
    for p in peers:
        send(k_send, k_recv.at[me], k_ss.at[p], k_rs.at[me], {"seq": p})
    k_recv[me] = k_send[...]

    windowed(spec_s)
    products(spec_u, True)
    for b in range(n):
        g_send[b] = (inverse(b) * scale).astype(BF16)

    def band(z):
        return pl.ds(pl.multiple_of(z * part, part), part)

    for k in range(nc - 2, -1, -1):
        z = zorder[k]
        send(g_send.at[:, band(z)], zg.at[mz], gz_ss.at[k], gz_rs.at[mz], {"chan": z})

    for q in [me] + peers:
        if q is not me:
            arrived(rf.at[q], f_ss.at[q], f_rs.at[q], {"seq": q})
        transform(spec_f, q, rf[q])
    windowed(spec_f)
    products(spec_s, False)
    outputs(0, True)
    products(spec_u, True)
    outputs(1, True)

    for q in [me] + peers:
        if q is not me:
            for j in range(2):
                piece = pl.ds(j * half, half)
                arrived(s1.at[q, piece], s1_ss.at[q, j], s1_rs.at[q, j], {"seq": q})
        transform(spec_s, q, s1[q])
    products(spec_s, False)
    outputs(2, False)

    for k in range(nc - 1):
        z = zorder[k]
        arrived(zg.at[z], gz_ss.at[k], gz_rs.at[z], {"chan": z})
    for p in range(n):
        acc = g_send[p, band(mz)].astype(F32)
        for z in zorder:
            acc += zg[z, p].astype(F32)
        g2_send[p] = acc.astype(BF16)
    for p in peers:
        send(g2_send.at[p], g2_recv.at[me], g2_ss.at[p], g2_rs.at[me], {"seq": p})
    g2_recv[me] = g2_send[me]
    give_back(2)

    loaded(skip, fq)
    for q in [me] + peers:
        at = lane(q)
        gain = skip[:, at]
        if q is not me:
            arrived(c_recv.at[0, q], c_ss.at[0, q], c_rs.at[0, q], {"seq": q})
        mixed = c_recv[0, q].astype(F32) + gain * su_send[q, 0].astype(F32)
        gq_o[:, at] = (bg[:, at].astype(F32) * mixed).astype(BF16)
    for q in peers:
        arrived(k_recv.at[q], k_ss.at[q], k_rs.at[q], {"seq": q})
    for q in range(n):
        gs_o[:, q * w:(q + 1) * w] = k_recv[q, 0:1]
    for q in [me] + peers:
        at = lane(q)
        gain = skip[:, at]
        if q is not me:
            arrived(c_recv.at[1, q], c_ss.at[1, q], c_rs.at[1, q], {"seq": q})
        through = c_recv[1, q].astype(F32) + gain * su_send[q, 1].astype(F32)
        gk_o[:, at] = (through * bv[:, at].astype(F32)).astype(BF16)
        gv_o[:, at] = (through * bk[:, at].astype(F32)).astype(BF16)
    for q in peers:
        arrived(g2_recv.at[q], g2_ss.at[q], g2_rs.at[q], {"seq": q})
    for k in range(nc - 2, -1, -1):
        z = zorder[k]
        send(g2_recv.at[pl.ds(z * per, per)], g3.at[mz], g3_ss.at[k], g3_rs.at[mz], {"chan": z})
    for h in range(per):
        g3[mz, h] = g2_recv[mz * per + h]
    for q in [me] + peers:
        at = lane(q)
        gain = skip[:, at]
        if q is not me:
            arrived(c_recv.at[2, q], c_ss.at[2, q], c_rs.at[2, q], {"seq": q})
        mixed = c_recv[2, q].astype(F32) + gain * s1_send[q].astype(F32)
        out_o[:, at] = (fq[:, at].astype(F32) * mixed).astype(BF16)
    for k in range(nc - 1):
        z = zorder[k]
        arrived(g3.at[z], g3_ss.at[k], g3_rs.at[z], {"chan": z})
    for z in range(nc):
        for h in range(per):
            gf_o[z * part:(z + 1) * part, h * w:(h + 1) * w] = g3[z, h].astype(F32)

    for c in started:
        c.wait_send()
    for p in peers:
        copy(fz.at[p], rf.at[me], f_ss.at[p], f_rs.at[me], {"seq": p}).wait_send()
    for k in range(nc - 1):
        @pl.when(near(zorder[k]))
        def _(k=k):
            for h in range(per):
                chan_copy(k, h).wait_send()
    for on, origin, to in relays:
        @pl.when(on)
        def _(origin=origin, to=to):
            for h in range(per):
                relay_copy(origin, h, to).wait_send()


def store_all(*refs):
    count = len(refs) // 2
    near, far, sems = refs[:count], refs[count:2 * count], refs[-1]
    stores = [pltpu.make_async_copy(near[i], far[i], sems.at[i]) for i in range(count)]
    for c in stores:
        c.start()
    for c in stores:
        c.wait()


def fused_device(n, nc, *args):
    fwd_q, filters, skip = args[0], args[7], args[8]
    rows, chan_width = fwd_q.shape
    w = chan_width // n
    per = filters.shape[1] // w
    part = rows // nc
    scale = 1.0 / math.sqrt(rows * n)
    forward, inverse = (jnp.asarray(t, dtype=BF16) for t in block_tables(rows))
    results = (
        *[pltpu.VMEM((rows, chan_width), BF16)] * 4, pltpu.VMEM(filters.shape, F32), pltpu.VMEM((1, chan_width), F32),
    )
    dma = pltpu.SemaphoreType.DMA
    block = (n, rows, w)
    spectrum = (n, 2 * rows, w)
    scratch = [
        *[pltpu.VMEM((rows, chan_width), BF16)] * 7, pltpu.VMEM(filters.shape, F32),
        pltpu.VMEM((1, chan_width), F32), pltpu.VMEM(forward.shape, BF16), pltpu.VMEM(inverse.shape, BF16),
        dma((11,)),
        pltpu.VMEM((n, 2, rows, w), BF16), pltpu.VMEM(block, BF16), pltpu.VMEM(block, BF16),
        pltpu.VMEM((n, 2, rows, w), BF16), pltpu.VMEM(block, BF16), pltpu.VMEM(block, BF16),
        *[pltpu.VMEM(spectrum, F32)] * 5,
        pltpu.VMEM((3,) + block, BF16), pltpu.VMEM((3,) + block, BF16),
        pltpu.VMEM(block, BF16), pltpu.VMEM((nc, n, part, w), BF16),
        pltpu.VMEM((n, part, w), BF16), pltpu.VMEM((n, part, w), BF16), pltpu.VMEM((nc, per, part, w), BF16),
        pltpu.VMEM((8, w), F32), pltpu.VMEM((n, 8, w), F32),
        dma((n,)), dma((n,)), dma((n, 2)), dma((n, 2)), dma((n,)), dma((n,)),
        dma((nc, per)), dma((nc, per)), dma((per,)), dma((3, n)), dma((3, n)),
        dma((nc,)), dma((nc,)), dma((n,)), dma((n,)), dma((nc,)), dma((nc,)), dma((n,)), dma((n,)),
    ]
    operands = (*args[:8], skip.reshape(1, chan_width), forward, inverse)
    hbm, vmem = (pl.BlockSpec(memory_space=m) for m in (pltpu.HBM, pltpu.VMEM))
    outs = pl.pallas_call(
        functools.partial(kernel, n, nc, scale),
        out_shape=results,
        in_specs=[hbm] * 11,
        out_specs=(vmem,) * 6,
        scratch_shapes=scratch,
        compiler_params=pltpu.CompilerParams(
            collective_id=0, has_side_effects=True, vmem_limit_bytes=KERNEL_VMEM
        ),
    )(*[pltpu.with_memory_space_constraint(a, pltpu.HBM) for a in operands])
    outs = pl.pallas_call(
        store_all,
        out_shape=tuple(jax.ShapeDtypeStruct(o.shape, o.dtype) for o in outs),
        in_specs=[vmem] * 6,
        out_specs=(hbm,) * 6,
        scratch_shapes=[dma((6,))],
        compiler_params=pltpu.CompilerParams(vmem_limit_bytes=KERNEL_VMEM),
    )(*outs)
    return tuple(outs[:5]) + (outs[5].reshape(chan_width),)


def routed(*args):
    n, nc = lax.axis_size("seq"), lax.axis_size("chan")
    rows, chan_width = args[0].shape
    filter_width = args[7].shape[1]
    fits = chan_width % (n * LANES) == 0 and rows % (16 * nc) == 0 and rows % 32 == 0
    fits = fits and n & (n - 1) == 0 and nc <= REACH + 2
    if fits and filter_width * nc == chan_width and filter_width % (chan_width // n) == 0:
        return fused_device(n, nc, *args)
    return per_device(*args)


def solution(mesh):
    return jax.shard_map(
        routed,
        mesh=mesh,
        in_specs=(
            P("seq", "chan"),
            P("seq", "chan"),
            P("seq", "chan"),
            P("seq", "chan"),
            P("seq", "chan"),
            P("seq", "chan"),
            P("seq", "chan"),
            P("seq", "chan"),
            P("chan"),
        ),
        out_specs=(
            P("seq", "chan"),
            P("seq", "chan"),
            P("seq", "chan"),
            P("seq", "chan"),
            P("seq", "chan"),
            P("chan"),
        ),
        check_vma=False,
    )
```

```python
import functools
import math

import jax
import jax.numpy as jnp
import numpy as np
from jax import lax
from jax.experimental import pallas as pl
from jax.experimental.pallas import tpu as pltpu
from jax.sharding import PartitionSpec as P

HIGHEST = lax.Precision.HIGHEST
LANES = 128
MESH = pl.DeviceIdType.MESH
BF16 = jnp.bfloat16
F32 = jnp.float32
KERNEL_VMEM = 32 * 2**20


def index_ramp(total):
    return jnp.arange(total, dtype=jnp.int32)


def widened(values):
    return values.astype(jnp.float32)


def angles(out_index, in_index, period, sign):
    phase_steps = out_index[:, None] * in_index[None, :] % period
    phase = phase_steps.astype(jnp.float32) * (sign * 2.0 * math.pi / period)
    return (jnp.cos(phase), jnp.sin(phase))


def times_table(left, right):
    return (left[0] * right[0] - left[1] * right[1], left[0] * right[1] + left[1] * right[0])


def block_table(pair):
    cosine, sine_part = pair
    return jnp.stack([jnp.stack([cosine, -sine_part]), jnp.stack([sine_part, cosine])])


def product_of(left, right):
    return jnp.stack(
        [left[0] * right[0] - left[1] * right[1], left[0] * right[1] + left[1] * right[0]]
    )


def conj_product(left, right):
    return jnp.stack(
        [left[0] * right[0] + left[1] * right[1], left[0] * right[1] - left[1] * right[0]]
    )


def joined(left, right):
    return jnp.concatenate([left, right], axis=-1)


def factor(total):
    chosen = 1
    for candidate in range(1, total + 1):
        if candidate * candidate <= total and total % candidate == 0:
            chosen = candidate
    return chosen


def leading_section(values, seq_size):
    cosine, sine_part = angles(index_ramp(2 * seq_size), index_ramp(seq_size), 2 * seq_size, -1.0)
    table = jnp.stack([cosine, sine_part])
    return jnp.einsum("rkp,pmc->rkmc", table, values, precision=HIGHEST)


def trailing_section(values, seq_size, period):
    cosine, sine_part = angles(index_ramp(seq_size), index_ramp(2 * seq_size), 2 * seq_size, 1.0)
    table = jnp.stack([cosine, -sine_part]) * (1.0 / period)
    return jnp.einsum("rpk,rkmc->pmc", table, values, precision=HIGHEST)


def inner_forward(values, freq_keys, period):
    lead_size, row_count, chan_count = values.shape[1:]
    outer_size = factor(row_count)
    inner_size = row_count // outer_size
    values = values.reshape(2, lead_size, outer_size, inner_size, chan_count)
    first_twiddle = angles(freq_keys, index_ramp(row_count), period, -1.0)
    first_twiddle = tuple(
        (part.reshape(lead_size, outer_size, inner_size) for part in first_twiddle)
    )
    outer_dft = angles(index_ramp(outer_size), index_ramp(outer_size), outer_size, -1.0)
    outer_table = times_table(
        tuple((part[None, :, :, None] for part in outer_dft)),
        tuple((part[:, None, :, :] for part in first_twiddle)),
    )
    values = jnp.einsum("rsjxab,sjabc->rjxbc", block_table(outer_table), values, precision=HIGHEST)
    second_twiddle = angles(index_ramp(outer_size), index_ramp(inner_size), row_count, -1.0)
    inner_dft = angles(index_ramp(inner_size), index_ramp(inner_size), inner_size, -1.0)
    inner_table = times_table(
        tuple((part[None, :, :] for part in inner_dft)),
        tuple((part[:, None, :] for part in second_twiddle)),
    )
    return jnp.einsum("rsxyb,sjxbc->rjxyc", block_table(inner_table), values, precision=HIGHEST)


def inner_inverse(values, freq_keys, period):
    lead_size, outer_size, inner_size, chan_count = values.shape[1:]
    row_count = outer_size * inner_size
    second_twiddle = angles(index_ramp(outer_size), index_ramp(inner_size), row_count, 1.0)
    inner_dft = angles(index_ramp(inner_size), index_ramp(inner_size), inner_size, 1.0)
    inner_table = times_table(
        tuple((part[:, :, None] for part in second_twiddle)),
        tuple((part[None, :, :] for part in inner_dft)),
    )
    values = jnp.einsum("rsxby,sjxyc->rjxbc", block_table(inner_table), values, precision=HIGHEST)
    first_twiddle = angles(freq_keys, index_ramp(row_count), period, 1.0)
    first_twiddle = tuple(
        (part.reshape(lead_size, outer_size, inner_size) for part in first_twiddle)
    )
    outer_dft = angles(index_ramp(outer_size), index_ramp(outer_size), outer_size, 1.0)
    outer_table = times_table(
        tuple((part[:, :, :, None] for part in first_twiddle)),
        tuple((part[None, :, None, :] for part in outer_dft)),
    )
    values = jnp.einsum("rsjabx,sjxbc->rjabc", block_table(outer_table), values, precision=HIGHEST)
    return values.reshape(2, lead_size, row_count, chan_count)


def forward_local(signal_part, seq_size):
    seq_length, chan_count = signal_part.shape
    row_count = seq_length // seq_size
    values = leading_section(signal_part.reshape(seq_size, row_count, chan_count), seq_size)
    return inner_forward(values, index_ramp(2 * seq_size), 2 * seq_length)


def inverse_local(values, seq_size):
    lead_size, outer_size, inner_size, chan_count = values.shape[1:]
    row_count = outer_size * inner_size
    period = 2 * seq_size * row_count
    values = inner_inverse(values, index_ramp(2 * seq_size), period)
    return trailing_section(values, seq_size, period).reshape(seq_size * row_count, chan_count)


def filter_times_pair(spec_filter, spec_pair):
    shape_pair = spec_pair.shape
    width = spec_filter.shape[-1]
    pair_view = spec_pair.reshape(shape_pair[:-1] + (2, width))
    filter_view = spec_filter[..., None, :]
    return product_of(filter_view, pair_view).reshape(shape_pair)


def per_device(fwd_q, fwd_k, fwd_v, bwd_q, bwd_k, bwd_v, bwd_grad, filters, skip):
    row_count, chan_width = fwd_q.shape
    seq_size = lax.axis_size("seq")
    grad_scale = 1.0 / math.sqrt(row_count * seq_size)
    source = (widened(fwd_k) * widened(fwd_v)).astype(jnp.bfloat16)
    second_source = (widened(bwd_k) * widened(bwd_v)).astype(jnp.bfloat16)
    upstream = (widened(bwd_grad) * widened(bwd_q)).astype(jnp.bfloat16)
    skip_gain = widened(skip)
    filters_all = lax.all_gather(filters, "chan", axis=1, tiled=True)
    narrow = chan_width // seq_size
    local_first, local_second = (
        lax.all_to_all(source, "seq", split_axis=1, concat_axis=0, tiled=True),
        lax.all_to_all(second_source, "seq", split_axis=1, concat_axis=0, tiled=True),
    )
    local_filter = lax.all_to_all(filters_all, "seq", split_axis=1, concat_axis=0, tiled=True)
    local_up = lax.all_to_all(upstream, "seq", split_axis=1, concat_axis=0, tiled=True)
    spec_sources = forward_local(
        widened(jnp.concatenate([local_first, local_second], axis=1)), seq_size
    )
    spec_filter = forward_local(local_filter, seq_size)
    conv_local = inverse_local(filter_times_pair(spec_filter, spec_sources), seq_size)
    conv_first, conv_second = (
        lax.all_to_all(conv_local[:, :narrow], "seq", split_axis=0, concat_axis=1, tiled=True),
        lax.all_to_all(conv_local[:, narrow:], "seq", split_axis=0, concat_axis=1, tiled=True),
    )
    spec_up = forward_local(widened(local_up), seq_size)
    spec_second = spec_sources[..., narrow:]
    back_local = inverse_local(
        joined(conj_product(spec_filter, spec_up), conj_product(spec_second, spec_up)), seq_size
    )
    through_conv, filter_terms = (
        lax.all_to_all(back_local[:, :narrow], "seq", split_axis=0, concat_axis=1, tiled=True),
        lax.all_to_all(
            back_local[:, narrow:] * grad_scale, "seq", split_axis=0, concat_axis=1, tiled=True
        ),
    )
    grad_filter = lax.psum_scatter(filter_terms, "chan", scatter_dimension=1, tiled=True)
    source_wide = widened(source)
    second_wide = widened(second_source)
    upstream_wide = widened(upstream)
    mixed = conv_first + skip_gain * source_wide
    output = (widened(fwd_q) * mixed).astype(jnp.bfloat16)
    mixed_two = conv_second + skip_gain * second_wide
    grad_query = (widened(bwd_grad) * mixed_two).astype(jnp.bfloat16)
    through = through_conv + skip_gain * upstream_wide
    grad_key = (through * widened(bwd_v)).astype(jnp.bfloat16)
    grad_value = (through * widened(bwd_k)).astype(jnp.bfloat16)
    grad_skip = lax.psum(jnp.sum(upstream_wide * second_wide, axis=0) * grad_scale, "seq")
    return (output, grad_query, grad_key, grad_value, grad_filter, grad_skip)


def block_tables(rows):
    freq = 2 * np.arange(rows)[:, None] + 1
    phase = (freq * np.arange(rows)[None, :] % (4 * rows)) * (np.pi / (2 * rows))
    forward = np.concatenate([np.cos(phase), -np.sin(phase)], axis=0)
    inverse = np.concatenate([np.cos(phase), -np.sin(phase)], axis=0).T / rows
    return forward.astype(np.float32), inverse.astype(np.float32)


REACH = 2


def kernel(
    n, nc, scale,
    fq_h, fk_h, fv_h, bq_h, bk_h, bv_h, bg_h, filt_h, skip_h, fwd_h, inv_h,
    out_o, gq_o, gk_o, gv_o, gf_o, gs_o,
    fq, fk, fv, bq, bk, bv, bg, filt, skip, fwd_t, inv_t, in_sem,
    su_send, s1_send, fz, su, s1, rf, spec_s, spec_u, spec_f, spec_w, prod,
    c_send, c_recv, g_send, zg, g2_send, g2_recv, g3, k_send, k_recv,
    su_ss, su_rs, s1_ss, s1_rs, f_ss, f_rs, z_ss, z_rs, credit, c_ss, c_rs,
    gz_ss, gz_rs, g2_ss, g2_rs, g3_ss, g3_rs, k_ss, k_rs,
):
    rows, chan_width = fq.shape
    w = chan_width // n
    per = filt.shape[1] // w
    part, half = rows // nc, rows // 2
    me = lax.axis_index("seq")
    mz = lax.axis_index("chan")

    def flipped(r):
        at, bit = me, 1
        while bit < n:
            if r & bit:
                at = at + bit * (1 - 2 * lax.rem(me // bit, 2))
            bit *= 2
        return at

    order = sorted(range(1, n), key=lambda r: (r & 1, -r))
    peers = [flipped(r) for r in order]
    upward = 2 * mz < nc
    zorder = []
    for k in range(nc - 1):
        j = nc - 1 - k
        zorder.append(jnp.where(upward, jnp.where(mz <= k, k + 1, k), jnp.where(mz >= j, j - 1, j)))

    def near(z):
        return (z - mz <= REACH) & (mz - z <= REACH)

    def lane(p):
        return pl.ds(pl.multiple_of(p * w, w), w)

    def copy(src, dst, ss, rs, to):
        return pltpu.make_async_remote_copy(
            src_ref=src, dst_ref=dst, send_sem=ss, recv_sem=rs, device_id=to, device_id_type=MESH
        )

    started = []

    def send(src, dst, ss, rs, to):
        c = copy(src, dst, ss, rs, to)
        c.start()
        started.append(c)

    def arrived(buf, ss, rs, to):
        copy(buf, buf, ss, rs, to).wait_recv()

    loads = {}
    order_in = ((filt_h, filt), (bk_h, bk), (bv_h, bv), (bg_h, bg), (bq_h, bq), (fk_h, fk), (fv_h, fv))
    for at, (far, dst) in enumerate(order_in + ((fwd_h, fwd_t), (inv_h, inv_t), (skip_h, skip), (fq_h, fq))):
        loads[id(dst)] = pltpu.make_async_copy(far, dst, in_sem.at[at])
        loads[id(dst)].start()

    def loaded(*refs):
        for ref in refs:
            loads[id(ref)].wait()

    barrier = pltpu.get_barrier_semaphore()
    for p in peers:
        pl.semaphore_signal(barrier, inc=1, device_id={"seq": p}, device_id_type=MESH)
    greeted = n - 1
    for z in zorder:
        greeted = greeted + near(z).astype(jnp.int32)

        @pl.when(near(z))
        def _(z=z):
            pl.semaphore_signal(barrier, inc=1, device_id={"chan": z}, device_id_type=MESH)

    def transform(dst, q, block):
        dst[q] = jnp.dot(fwd_t[...], block, preferred_element_type=F32)

    loaded(filt)
    for h in range(per):
        fz[mz * per + h] = filt[:, h * w:(h + 1) * w].astype(BF16)
    loaded(bk, bv, bg, bq)
    for p in range(n):
        cols = slice(p * w, (p + 1) * w)
        su_send[p, 0] = (bk[:, cols].astype(F32) * bv[:, cols].astype(F32)).astype(BF16)
        su_send[p, 1] = (bg[:, cols].astype(F32) * bq[:, cols].astype(F32)).astype(BF16)
    pl.semaphore_wait(barrier, greeted)

    def chan_copy(k, h):
        block = fz.at[mz * per + h]
        return copy(block, block, z_ss.at[k, h], z_rs.at[mz, h], {"chan": zorder[k]})

    def forward(o, h):
        p = o * per + h

        @pl.when(p != me)
        def _():
            copy(fz.at[p], rf.at[me], f_ss.at[p], f_rs.at[me], {"seq": p}).start()

    def chan_send(k):
        for h in range(per):
            chan_copy(k, h).start()

    distant = ~near(zorder[-1]) if nc > 1 else None
    if nc > 1:
        o = zorder[-1]
        other = jnp.where(o > mz, mz - 1, mz + 1)
        vouch = ((o - mz == REACH) | (mz - o == REACH)) & (other >= 0) & (other < nc)

        @pl.when(vouch)
        def _():
            pl.semaphore_signal(credit, inc=1, device_id={"chan": o}, device_id_type=MESH)

        @pl.when(~distant)
        def _():
            for k in range(nc - 2, -1, -1):
                chan_send(k)

        @pl.when(distant)
        def _():
            for k in range(nc - 3, 0, -1):
                chan_send(k)

    for p in peers:
        send(su_send.at[p], su.at[me], su_ss.at[p], su_rs.at[me], {"seq": p})
    for h in range(per):
        forward(mz, h)

    loaded(fk, fv)
    for p in range(n):
        cols = slice(p * w, (p + 1) * w)
        s1_send[p] = (fk[:, cols].astype(F32) * fv[:, cols].astype(F32)).astype(BF16)
    su[me] = su_send[me]
    s1[me] = s1_send[me]
    loaded(fwd_t, inv_t)
    transform(spec_s, me, su[me, 0])
    transform(spec_u, me, su[me, 1])

    if nc > 1:
        @pl.when(distant)
        def _():
            pl.semaphore_wait(credit, 1)
            chan_send(nc - 2)
            chan_send(0)

    for k in range(nc - 1):
        o = zorder[k]
        for h in range(per):
            arrived(fz.at[o * per + h], z_ss.at[k, h], z_rs.at[o, h], {"chan": o})
            forward(o, h)
    rf[me] = fz[me]
    for p in peers:
        send(s1_send.at[p], s1.at[me], s1_ss.at[p], s1_rs.at[me], {"seq": p})

    sign = 1.0 - 2.0 * lax.rem(lax.broadcasted_iota(jnp.int32, (rows, w), 0), 2).astype(F32)

    def windowed(src):
        spec_w[0] = src[0]
        for d in range(1, n):
            spec_w[d, :rows] = src[d, :rows] - sign * src[d - 1, rows:]
            spec_w[d, rows:] = src[d, rows:] + sign * src[d - 1, :rows]

    def products(src, corr):
        def tile(k, carry):
            re_at = pl.ds(pl.multiple_of(k * 8, 8), 8)
            im_at = pl.ds(pl.multiple_of(rows + k * 8, 8), 8)
            ar = [spec_w[d, re_at] for d in range(n)]
            ai = [spec_w[d, im_at] for d in range(n)]
            xr = [src[d, re_at] for d in range(n)]
            xi = [src[d, im_at] for d in range(n)]
            for b in range(n):
                terms = [(c - b, c) for c in range(b, n)] if corr else [(b - c, c) for c in range(b + 1)]
                re, im = None, None
                for d, c in terms:
                    if corr:
                        tr = ar[d] * xr[c] + ai[d] * xi[c]
                        ti = ar[d] * xi[c] - ai[d] * xr[c]
                    else:
                        tr = ar[d] * xr[c] - ai[d] * xi[c]
                        ti = ar[d] * xi[c] + ai[d] * xr[c]
                    re = tr if re is None else re + tr
                    im = ti if im is None else im + ti
                prod[b, re_at] = re
                prod[b, im_at] = im
            return carry

        lax.fori_loop(0, rows // 8, tile, 0)

    def inverse(b):
        return jnp.dot(inv_t[...], prod[b].astype(BF16), preferred_element_type=F32)

    def batches(items):
        return [items[:n // 2], items[n // 2:]]

    def give_back(which, group):
        for p in group:
            send(c_send.at[which, p], c_recv.at[which, me], c_ss.at[which, p], c_rs.at[which, me], {"seq": p})

    def outputs(which, now):
        for group in batches(peers):
            for p in group:
                c_send[which, p] = inverse(p).astype(BF16)
            give_back(which, [p for p in group if any(p is x for x in now)])
        c_recv[which, me] = inverse(me).astype(BF16)

    for group in batches(peers):
        for q in group:
            arrived(su.at[q], su_ss.at[q], su_rs.at[q], {"seq": q})
        for q in group:
            transform(spec_s, q, su[q, 0])
            transform(spec_u, q, su[q, 1])
    total = jnp.zeros((1, w), F32)
    for q in range(n):
        total += jnp.sum(su[q, 0].astype(F32) * su[q, 1].astype(F32), axis=0, keepdims=True)
    k_send[...] = jnp.broadcast_to(total * scale, k_send.shape)
    for p in peers:
        send(k_send, k_recv.at[me], k_ss.at[p], k_rs.at[me], {"seq": p})
    k_recv[me] = k_send[...]

    windowed(spec_s)
    products(spec_u, True)
    for b in range(n):
        g_send[b] = (inverse(b) * scale).astype(BF16)

    def band(z):
        return pl.ds(pl.multiple_of(z * part, part), part)

    for k in range(nc - 2, -1, -1):
        z = zorder[k]
        send(g_send.at[:, band(z)], zg.at[mz], gz_ss.at[k], gz_rs.at[mz], {"chan": z})

    transform(spec_f, me, rf[me])
    for group in batches(peers):
        for q in group:
            arrived(rf.at[q], f_ss.at[q], f_rs.at[q], {"seq": q})
        for q in group:
            transform(spec_f, q, rf[q])
    windowed(spec_f)
    products(spec_s, False)
    outputs(0, peers)
    products(spec_u, True)
    outputs(1, batches(peers)[0])

    for q in peers:
        arrived(s1.at[q], s1_ss.at[q], s1_rs.at[q], {"seq": q})
    for q in range(n):
        transform(spec_s, q, s1[q])
    products(spec_s, False)
    outputs(2, [])

    for k in range(nc - 1):
        z = zorder[k]
        arrived(zg.at[z], gz_ss.at[k], gz_rs.at[z], {"chan": z})
    for p in range(n):
        acc = g_send[p, band(mz)].astype(F32)
        for z in zorder:
            acc += zg[z, p].astype(F32)
        g2_send[p] = acc.astype(BF16)
    for p in peers:
        send(g2_send.at[p], g2_recv.at[me], g2_ss.at[p], g2_rs.at[me], {"seq": p})
    g2_recv[me] = g2_send[me]
    give_back(1, batches(peers)[1])
    give_back(2, peers)

    loaded(skip, fq)
    for q in [me] + peers:
        at = lane(q)
        gain = skip[:, at]
        if q is not me:
            arrived(c_recv.at[0, q], c_ss.at[0, q], c_rs.at[0, q], {"seq": q})
        mixed = c_recv[0, q].astype(F32) + gain * su_send[q, 0].astype(F32)
        gq_o[:, at] = (bg[:, at].astype(F32) * mixed).astype(BF16)
    for q in peers:
        arrived(g2_recv.at[q], g2_ss.at[q], g2_rs.at[q], {"seq": q})
    for k in range(nc - 2, -1, -1):
        z = zorder[k]
        send(g2_recv.at[pl.ds(z * per, per)], g3.at[mz], g3_ss.at[k], g3_rs.at[mz], {"chan": z})
    for h in range(per):
        g3[mz, h] = g2_recv[mz * per + h]
    for q in peers:
        arrived(k_recv.at[q], k_ss.at[q], k_rs.at[q], {"seq": q})
    for q in range(n):
        gs_o[:, q * w:(q + 1) * w] = k_recv[q, 0:1]
    for q in [me] + peers:
        at = lane(q)
        gain = skip[:, at]
        if q is not me:
            arrived(c_recv.at[1, q], c_ss.at[1, q], c_rs.at[1, q], {"seq": q})
        through = c_recv[1, q].astype(F32) + gain * su_send[q, 1].astype(F32)
        gk_o[:, at] = (through * bv[:, at].astype(F32)).astype(BF16)
        gv_o[:, at] = (through * bk[:, at].astype(F32)).astype(BF16)
    for q in [me] + peers:
        at = lane(q)
        gain = skip[:, at]
        if q is not me:
            arrived(c_recv.at[2, q], c_ss.at[2, q], c_rs.at[2, q], {"seq": q})
        mixed = c_recv[2, q].astype(F32) + gain * s1_send[q].astype(F32)
        out_o[:, at] = (fq[:, at].astype(F32) * mixed).astype(BF16)
    for k in range(nc - 1):
        z = zorder[k]
        arrived(g3.at[z], g3_ss.at[k], g3_rs.at[z], {"chan": z})
    for z in range(nc):
        for h in range(per):
            gf_o[z * part:(z + 1) * part, h * w:(h + 1) * w] = g3[z, h].astype(F32)

    for c in started:
        c.wait_send()
    for p in peers:
        copy(fz.at[p], rf.at[me], f_ss.at[p], f_rs.at[me], {"seq": p}).wait_send()
    for k in range(nc - 1):
        for h in range(per):
            chan_copy(k, h).wait_send()


def store_all(*refs):
    count = len(refs) // 2
    near, far, sems = refs[:count], refs[count:2 * count], refs[-1]
    stores = [pltpu.make_async_copy(near[i], far[i], sems.at[i]) for i in range(count)]
    for c in stores:
        c.start()
    for c in stores:
        c.wait()


def fused_device(n, nc, *args):
    fwd_q, filters, skip = args[0], args[7], args[8]
    rows, chan_width = fwd_q.shape
    w = chan_width // n
    per = filters.shape[1] // w
    part = rows // nc
    scale = 1.0 / math.sqrt(rows * n)
    forward, inverse = (jnp.asarray(t, dtype=BF16) for t in block_tables(rows))
    results = (
        *[pltpu.VMEM((rows, chan_width), BF16)] * 4, pltpu.VMEM(filters.shape, F32), pltpu.VMEM((1, chan_width), F32),
    )
    dma = pltpu.SemaphoreType.DMA
    block = (n, rows, w)
    spectrum = (n, 2 * rows, w)
    scratch = [
        *[pltpu.VMEM((rows, chan_width), BF16)] * 7, pltpu.VMEM(filters.shape, F32),
        pltpu.VMEM((1, chan_width), F32), pltpu.VMEM(forward.shape, BF16), pltpu.VMEM(inverse.shape, BF16),
        dma((11,)),
        pltpu.VMEM((n, 2, rows, w), BF16), pltpu.VMEM(block, BF16), pltpu.VMEM(block, BF16),
        pltpu.VMEM((n, 2, rows, w), BF16), pltpu.VMEM(block, BF16), pltpu.VMEM(block, BF16),
        *[pltpu.VMEM(spectrum, F32)] * 5,
        pltpu.VMEM((3,) + block, BF16), pltpu.VMEM((3,) + block, BF16),
        pltpu.VMEM(block, BF16), pltpu.VMEM((nc, n, part, w), BF16),
        pltpu.VMEM((n, part, w), BF16), pltpu.VMEM((n, part, w), BF16), pltpu.VMEM((nc, per, part, w), BF16),
        pltpu.VMEM((8, w), F32), pltpu.VMEM((n, 8, w), F32),
        dma((n,)), dma((n,)), dma((n,)), dma((n,)), dma((n,)), dma((n,)),
        dma((nc, per)), dma((nc, per)), pltpu.SemaphoreType.REGULAR, dma((3, n)), dma((3, n)),
        dma((nc,)), dma((nc,)), dma((n,)), dma((n,)), dma((nc,)), dma((nc,)), dma((n,)), dma((n,)),
    ]
    operands = (*args[:8], skip.reshape(1, chan_width), forward, inverse)
    hbm, vmem = (pl.BlockSpec(memory_space=m) for m in (pltpu.HBM, pltpu.VMEM))
    outs = pl.pallas_call(
        functools.partial(kernel, n, nc, scale),
        out_shape=results,
        in_specs=[hbm] * 11,
        out_specs=(vmem,) * 6,
        scratch_shapes=scratch,
        compiler_params=pltpu.CompilerParams(
            collective_id=0, has_side_effects=True, vmem_limit_bytes=KERNEL_VMEM
        ),
    )(*[pltpu.with_memory_space_constraint(a, pltpu.HBM) for a in operands])
    outs = pl.pallas_call(
        store_all,
        out_shape=tuple(jax.ShapeDtypeStruct(o.shape, o.dtype) for o in outs),
        in_specs=[vmem] * 6,
        out_specs=(hbm,) * 6,
        scratch_shapes=[dma((6,))],
        compiler_params=pltpu.CompilerParams(vmem_limit_bytes=KERNEL_VMEM),
    )(*outs)
    return tuple(outs[:5]) + (outs[5].reshape(chan_width),)


def routed(*args):
    n, nc = lax.axis_size("seq"), lax.axis_size("chan")
    rows, chan_width = args[0].shape
    filter_width = args[7].shape[1]
    fits = chan_width % (n * LANES) == 0 and rows % (16 * nc) == 0 and rows % 32 == 0
    fits = fits and n & (n - 1) == 0 and nc <= REACH + 2
    if fits and filter_width * nc == chan_width and filter_width % (chan_width // n) == 0:
        return fused_device(n, nc, *args)
    return per_device(*args)


def solution(mesh):
    return jax.shard_map(
        routed,
        mesh=mesh,
        in_specs=(
            P("seq", "chan"),
            P("seq", "chan"),
            P("seq", "chan"),
            P("seq", "chan"),
            P("seq", "chan"),
            P("seq", "chan"),
            P("seq", "chan"),
            P("seq", "chan"),
            P("chan"),
        ),
        out_specs=(
            P("seq", "chan"),
            P("seq", "chan"),
            P("seq", "chan"),
            P("seq", "chan"),
            P("seq", "chan"),
            P("chan"),
        ),
        check_vma=False,
    )
```

```python
import functools
import math

import jax
import jax.numpy as jnp
import numpy as np
from jax import lax
from jax.experimental import pallas as pl
from jax.experimental.pallas import tpu as pltpu
from jax.sharding import PartitionSpec as P

HIGHEST = lax.Precision.HIGHEST
LANES = 128
MESH = pl.DeviceIdType.MESH
BF16 = jnp.bfloat16
F32 = jnp.float32
KERNEL_VMEM = 32 * 2**20


def index_ramp(total):
    return jnp.arange(total, dtype=jnp.int32)


def widened(values):
    return values.astype(jnp.float32)


def angles(out_index, in_index, period, sign):
    phase_steps = out_index[:, None] * in_index[None, :] % period
    phase = phase_steps.astype(jnp.float32) * (sign * 2.0 * math.pi / period)
    return (jnp.cos(phase), jnp.sin(phase))


def times_table(left, right):
    return (left[0] * right[0] - left[1] * right[1], left[0] * right[1] + left[1] * right[0])


def block_table(pair):
    cosine, sine_part = pair
    return jnp.stack([jnp.stack([cosine, -sine_part]), jnp.stack([sine_part, cosine])])


def product_of(left, right):
    return jnp.stack(
        [left[0] * right[0] - left[1] * right[1], left[0] * right[1] + left[1] * right[0]]
    )


def conj_product(left, right):
    return jnp.stack(
        [left[0] * right[0] + left[1] * right[1], left[0] * right[1] - left[1] * right[0]]
    )


def joined(left, right):
    return jnp.concatenate([left, right], axis=-1)


def factor(total):
    chosen = 1
    for candidate in range(1, total + 1):
        if candidate * candidate <= total and total % candidate == 0:
            chosen = candidate
    return chosen


def leading_section(values, seq_size):
    cosine, sine_part = angles(index_ramp(2 * seq_size), index_ramp(seq_size), 2 * seq_size, -1.0)
    table = jnp.stack([cosine, sine_part])
    return jnp.einsum("rkp,pmc->rkmc", table, values, precision=HIGHEST)


def trailing_section(values, seq_size, period):
    cosine, sine_part = angles(index_ramp(seq_size), index_ramp(2 * seq_size), 2 * seq_size, 1.0)
    table = jnp.stack([cosine, -sine_part]) * (1.0 / period)
    return jnp.einsum("rpk,rkmc->pmc", table, values, precision=HIGHEST)


def inner_forward(values, freq_keys, period):
    lead_size, row_count, chan_count = values.shape[1:]
    outer_size = factor(row_count)
    inner_size = row_count // outer_size
    values = values.reshape(2, lead_size, outer_size, inner_size, chan_count)
    first_twiddle = angles(freq_keys, index_ramp(row_count), period, -1.0)
    first_twiddle = tuple(
        (part.reshape(lead_size, outer_size, inner_size) for part in first_twiddle)
    )
    outer_dft = angles(index_ramp(outer_size), index_ramp(outer_size), outer_size, -1.0)
    outer_table = times_table(
        tuple((part[None, :, :, None] for part in outer_dft)),
        tuple((part[:, None, :, :] for part in first_twiddle)),
    )
    values = jnp.einsum("rsjxab,sjabc->rjxbc", block_table(outer_table), values, precision=HIGHEST)
    second_twiddle = angles(index_ramp(outer_size), index_ramp(inner_size), row_count, -1.0)
    inner_dft = angles(index_ramp(inner_size), index_ramp(inner_size), inner_size, -1.0)
    inner_table = times_table(
        tuple((part[None, :, :] for part in inner_dft)),
        tuple((part[:, None, :] for part in second_twiddle)),
    )
    return jnp.einsum("rsxyb,sjxbc->rjxyc", block_table(inner_table), values, precision=HIGHEST)


def inner_inverse(values, freq_keys, period):
    lead_size, outer_size, inner_size, chan_count = values.shape[1:]
    row_count = outer_size * inner_size
    second_twiddle = angles(index_ramp(outer_size), index_ramp(inner_size), row_count, 1.0)
    inner_dft = angles(index_ramp(inner_size), index_ramp(inner_size), inner_size, 1.0)
    inner_table = times_table(
        tuple((part[:, :, None] for part in second_twiddle)),
        tuple((part[None, :, :] for part in inner_dft)),
    )
    values = jnp.einsum("rsxby,sjxyc->rjxbc", block_table(inner_table), values, precision=HIGHEST)
    first_twiddle = angles(freq_keys, index_ramp(row_count), period, 1.0)
    first_twiddle = tuple(
        (part.reshape(lead_size, outer_size, inner_size) for part in first_twiddle)
    )
    outer_dft = angles(index_ramp(outer_size), index_ramp(outer_size), outer_size, 1.0)
    outer_table = times_table(
        tuple((part[:, :, :, None] for part in first_twiddle)),
        tuple((part[None, :, None, :] for part in outer_dft)),
    )
    values = jnp.einsum("rsjabx,sjxbc->rjabc", block_table(outer_table), values, precision=HIGHEST)
    return values.reshape(2, lead_size, row_count, chan_count)


def forward_local(signal_part, seq_size):
    seq_length, chan_count = signal_part.shape
    row_count = seq_length // seq_size
    values = leading_section(signal_part.reshape(seq_size, row_count, chan_count), seq_size)
    return inner_forward(values, index_ramp(2 * seq_size), 2 * seq_length)


def inverse_local(values, seq_size):
    lead_size, outer_size, inner_size, chan_count = values.shape[1:]
    row_count = outer_size * inner_size
    period = 2 * seq_size * row_count
    values = inner_inverse(values, index_ramp(2 * seq_size), period)
    return trailing_section(values, seq_size, period).reshape(seq_size * row_count, chan_count)


def filter_times_pair(spec_filter, spec_pair):
    shape_pair = spec_pair.shape
    width = spec_filter.shape[-1]
    pair_view = spec_pair.reshape(shape_pair[:-1] + (2, width))
    filter_view = spec_filter[..., None, :]
    return product_of(filter_view, pair_view).reshape(shape_pair)


def per_device(fwd_q, fwd_k, fwd_v, bwd_q, bwd_k, bwd_v, bwd_grad, filters, skip):
    row_count, chan_width = fwd_q.shape
    seq_size = lax.axis_size("seq")
    grad_scale = 1.0 / math.sqrt(row_count * seq_size)
    source = (widened(fwd_k) * widened(fwd_v)).astype(jnp.bfloat16)
    second_source = (widened(bwd_k) * widened(bwd_v)).astype(jnp.bfloat16)
    upstream = (widened(bwd_grad) * widened(bwd_q)).astype(jnp.bfloat16)
    skip_gain = widened(skip)
    filters_all = lax.all_gather(filters, "chan", axis=1, tiled=True)
    narrow = chan_width // seq_size
    local_first, local_second = (
        lax.all_to_all(source, "seq", split_axis=1, concat_axis=0, tiled=True),
        lax.all_to_all(second_source, "seq", split_axis=1, concat_axis=0, tiled=True),
    )
    local_filter = lax.all_to_all(filters_all, "seq", split_axis=1, concat_axis=0, tiled=True)
    local_up = lax.all_to_all(upstream, "seq", split_axis=1, concat_axis=0, tiled=True)
    spec_sources = forward_local(
        widened(jnp.concatenate([local_first, local_second], axis=1)), seq_size
    )
    spec_filter = forward_local(local_filter, seq_size)
    conv_local = inverse_local(filter_times_pair(spec_filter, spec_sources), seq_size)
    conv_first, conv_second = (
        lax.all_to_all(conv_local[:, :narrow], "seq", split_axis=0, concat_axis=1, tiled=True),
        lax.all_to_all(conv_local[:, narrow:], "seq", split_axis=0, concat_axis=1, tiled=True),
    )
    spec_up = forward_local(widened(local_up), seq_size)
    spec_second = spec_sources[..., narrow:]
    back_local = inverse_local(
        joined(conj_product(spec_filter, spec_up), conj_product(spec_second, spec_up)), seq_size
    )
    through_conv, filter_terms = (
        lax.all_to_all(back_local[:, :narrow], "seq", split_axis=0, concat_axis=1, tiled=True),
        lax.all_to_all(
            back_local[:, narrow:] * grad_scale, "seq", split_axis=0, concat_axis=1, tiled=True
        ),
    )
    grad_filter = lax.psum_scatter(filter_terms, "chan", scatter_dimension=1, tiled=True)
    source_wide = widened(source)
    second_wide = widened(second_source)
    upstream_wide = widened(upstream)
    mixed = conv_first + skip_gain * source_wide
    output = (widened(fwd_q) * mixed).astype(jnp.bfloat16)
    mixed_two = conv_second + skip_gain * second_wide
    grad_query = (widened(bwd_grad) * mixed_two).astype(jnp.bfloat16)
    through = through_conv + skip_gain * upstream_wide
    grad_key = (through * widened(bwd_v)).astype(jnp.bfloat16)
    grad_value = (through * widened(bwd_k)).astype(jnp.bfloat16)
    grad_skip = lax.psum(jnp.sum(upstream_wide * second_wide, axis=0) * grad_scale, "seq")
    return (output, grad_query, grad_key, grad_value, grad_filter, grad_skip)


def block_tables(rows):
    freq = 2 * np.arange(rows)[:, None] + 1
    phase = (freq * np.arange(rows)[None, :] % (4 * rows)) * (np.pi / (2 * rows))
    forward = np.concatenate([np.cos(phase), -np.sin(phase)], axis=0)
    inverse = np.concatenate([np.cos(phase), -np.sin(phase)], axis=0).T / rows
    return forward.astype(np.float32), inverse.astype(np.float32)


REACH = 2


def kernel(
    n, nc, scale,
    fq_h, fk_h, fv_h, bq_h, bk_h, bv_h, bg_h, filt_h, skip_h, fwd_h, inv_h,
    out_o, gq_o, gk_o, gv_o, gf_o, gs_o,
    fq, fk, fv, bq, bk, bv, bg, filt, skip, fwd_t, inv_t, in_sem,
    s2_send, up_send, s1_send, fz, s2, up, s1, rf, spec_s, spec_u, spec_f, spec_w, prod,
    c_send, c_recv, g_send, zg, g2_send, g2_recv, g3, k_send, k_recv,
    in_ss, s2_rs, up_rs, s1_rs, f_ss, f_rs, z_ss, z_rs, credit, c_ss, c_rs,
    gz_ss, gz_rs, g2_ss, g2_rs, g3_ss, g3_rs, k_ss, k_rs,
):
    rows, chan_width = fq.shape
    w = chan_width // n
    per = filt.shape[1] // w
    part, half = rows // nc, rows // 2
    me = lax.axis_index("seq")
    mz = lax.axis_index("chan")

    def flipped(r):
        at, bit = me, 1
        while bit < n:
            if r & bit:
                at = at + bit * (1 - 2 * lax.rem(me // bit, 2))
            bit *= 2
        return at

    order = sorted(range(1, n), key=lambda r: (r & 1, -r))
    peers = [flipped(r) for r in order]
    paired = list(zip(order, peers))
    upward = 2 * mz < nc
    zorder = []
    for k in range(nc - 1):
        j = nc - 1 - k
        zorder.append(jnp.where(upward, jnp.where(mz <= k, k + 1, k), jnp.where(mz >= j, j - 1, j)))

    def near(z):
        return (z - mz <= REACH) & (mz - z <= REACH)

    def lane(p):
        return pl.ds(pl.multiple_of(p * w, w), w)

    def copy(src, dst, ss, rs, to):
        return pltpu.make_async_remote_copy(
            src_ref=src, dst_ref=dst, send_sem=ss, recv_sem=rs, device_id=to, device_id_type=MESH
        )

    def send(src, dst, ss, rs, to):
        copy(src, dst, ss, rs, to).start()

    def arrived(buf, rs):
        copy(buf, buf, rs, rs, {"seq": peers[0]}).wait_recv()

    def sent(buf, ss):
        copy(buf, buf, ss, ss, {"seq": peers[0]}).wait_send()

    span, count = 2 * rows, n // 2
    near_side = 2 * (count // 2)

    def side(r):
        return 1 if r >= near_side else 0

    offsets = (range(1, near_side), range(max(near_side, 1), n))

    loads = {}
    order_in = ((bk_h, bk), (bv_h, bv), (filt_h, filt), (bg_h, bg), (bq_h, bq), (fk_h, fk), (fv_h, fv))
    for at, (far, dst) in enumerate(order_in + ((fwd_h, fwd_t), (inv_h, inv_t), (skip_h, skip), (fq_h, fq))):
        loads[id(dst)] = pltpu.make_async_copy(far, dst, in_sem.at[at])
        loads[id(dst)].start()

    def loaded(*refs):
        for ref in refs:
            loads[id(ref)].wait()

    barrier = pltpu.get_barrier_semaphore()
    for p in peers:
        pl.semaphore_signal(barrier, inc=1, device_id={"seq": p}, device_id_type=MESH)
    greeted = n - 1
    for z in zorder:
        greeted = greeted + near(z).astype(jnp.int32)

        @pl.when(near(z))
        def _(z=z):
            pl.semaphore_signal(barrier, inc=1, device_id={"chan": z}, device_id_type=MESH)

    chips = [flipped(r) // 2 for r in range(n - 2, 0, -2)] + [me // 2]

    def transform(dst, c, src):
        block = jnp.concatenate([src[2 * c], src[2 * c + 1]], axis=0)
        dst[c] = jnp.dot(fwd_t[...], block, preferred_element_type=F32)

    def gated(dst, left, right):
        for p in range(n):
            cols = slice(p * w, (p + 1) * w)
            dst[p] = (left[:, cols].astype(F32) * right[:, cols].astype(F32)).astype(BF16)

    loaded(bk, bv)
    gated(s2_send, bk, bv)
    loaded(filt)
    for h in range(per):
        fz[mz * per + h] = filt[:, h * w:(h + 1) * w].astype(BF16)
    pl.semaphore_wait(barrier, greeted)

    def forward(o, h):
        p = o * per + h

        @pl.when(p != me)
        def _():
            away = jnp.where(p // near_side == me // near_side, 0, 1) if near_side else 1
            send(fz.at[p], rf.at[me], f_ss, f_rs.at[away], {"seq": p})

    def chan_send(k):
        block = fz.at[pl.ds(mz * per, per)]
        send(block, block, z_ss, z_rs.at[mz], {"chan": zorder[k]})

    distant = ~near(zorder[-1]) if nc > 1 else None
    if nc > 1:
        o = zorder[-1]
        other = jnp.where(o > mz, mz - 1, mz + 1)
        vouch = ((o - mz == REACH) | (mz - o == REACH)) & (other >= 0) & (other < nc)

        @pl.when(vouch)
        def _():
            pl.semaphore_signal(credit, inc=1, device_id={"chan": o}, device_id_type=MESH)

        @pl.when(~distant)
        def _():
            for k in range(nc - 2, -1, -1):
                chan_send(k)

        @pl.when(distant)
        def _():
            for k in range(nc - 3, -1, -1):
                chan_send(k)

    def scatter(src, dst, ss, rs):
        for r, p in paired:
            send(src.at[p], dst.at[me], ss, rs.at[side(r)], {"seq": p})
        dst[me] = src[me]

    scatter(s2_send, s2, in_ss, s2_rs)
    loaded(bg, bq)
    gated(up_send, bg, bq)
    scatter(up_send, up, in_ss, up_rs)
    loaded(fk, fv)
    gated(s1_send, fk, fv)
    loaded(fwd_t, inv_t)

    if nc > 1:
        @pl.when(distant)
        def _():
            pl.semaphore_wait(credit, 1)
            chan_send(nc - 2)

    for k in range(nc - 1):
        o = zorder[k]
        arrived(fz.at[pl.ds(o * per, per)], z_rs.at[o])
        for h in range(per):
            if k == 0:
                forward(mz, h)
            forward(o, h)
    for h in range(per if nc == 1 else 0):
        forward(mz, h)
    rf[me] = fz[me]

    sign = 1.0 - 2.0 * lax.rem(lax.broadcasted_iota(jnp.int32, (span, w), 0), 2).astype(F32)

    def windowed(src):
        spec_w[0] = src[0]
        for d in range(1, count):
            spec_w[d, :span] = src[d, :span] - sign * src[d - 1, span:]
            spec_w[d, span:] = src[d, span:] + sign * src[d - 1, :span]

    def products(src, corr):
        def tile(k, carry):
            re_at = pl.ds(pl.multiple_of(k * 16, 16), 16)
            im_at = pl.ds(pl.multiple_of(span + k * 16, 16), 16)
            ar = [spec_w[d, re_at] for d in range(count)]
            ai = [spec_w[d, im_at] for d in range(count)]
            xr = [src[d, re_at] for d in range(count)]
            xi = [src[d, im_at] for d in range(count)]
            for b in range(count):
                terms = [(c - b, c) for c in range(b, count)] if corr else [(b - c, c) for c in range(b + 1)]
                re, im = None, None
                for d, c in terms:
                    if corr:
                        tr = ar[d] * xr[c] + ai[d] * xi[c]
                        ti = ar[d] * xi[c] - ai[d] * xr[c]
                    else:
                        tr = ar[d] * xr[c] - ai[d] * xi[c]
                        ti = ar[d] * xi[c] + ai[d] * xr[c]
                    re = tr if re is None else re + tr
                    im = ti if im is None else im + ti
                prod[b, re_at] = re
                prod[b, im_at] = im
            return carry

        lax.fori_loop(0, span // 16, tile, 0)

    def inverse(b):
        return jnp.dot(inv_t[...], prod[b].astype(BF16), preferred_element_type=F32)

    def give_back(which, group):
        for r in group:
            p = flipped(r)
            send(c_send.at[which, p], c_recv.at[which, me], c_ss, c_rs.at[which, side(r)], {"seq": p})

    def halves(dst, c, value):
        dst[2 * c] = value[:rows].astype(BF16)
        dst[2 * c + 1] = value[rows:].astype(BF16)

    def batches(items):
        return [items[:len(items) // 2], items[len(items) // 2:]]

    def outputs(which, now):
        for group in batches(list(range(count))):
            for i in group:
                halves(c_send.at[which], chips[i], inverse(chips[i]))
            if now:
                give_back(which, [r for i in group for r in (n - 2 - 2 * i, n - 1 - 2 * i) if r])
        c_recv[which, me] = c_send[which, me]

    def gather(bufs, rs, specs):
        for at, group in enumerate(batches(list(range(count))[::-1])):
            for buf, sems in zip(bufs, rs):
                if len(offsets[at]):
                    arrived(buf.at[pl.ds(0, len(offsets[at]))], sems.at[at])
            for buf, spec in zip(bufs, specs):
                for i in group:
                    transform(spec, chips[i], buf)

    gather((s2, up), (s2_rs, up_rs), (spec_s, spec_u))
    scatter(s1_send, s1, in_ss, s1_rs)
    windowed(spec_s)
    products(spec_u, True)
    for b in range(count):
        halves(g_send, b, inverse(b) * scale)

    def place(z):
        return jnp.where(mz > z, mz - 1, mz)

    def band(z):
        return pl.ds(pl.multiple_of(z * part, part), part)

    for k in range(nc - 2, -1, -1):
        z = zorder[k]
        send(g_send.at[:, band(z)], zg.at[place(z)], gz_ss, gz_rs, {"chan": z})

    total = jnp.zeros((1, w), F32)
    for q in range(n):
        total += jnp.sum(s2[q].astype(F32) * up[q].astype(F32), axis=0, keepdims=True)
    k_send[...] = jnp.broadcast_to(total * scale, k_send.shape)
    for p in peers:
        send(k_send, k_recv.at[me], k_ss, k_rs, {"seq": p})
    k_recv[me] = k_send[...]

    gather((rf,), (f_rs,), (spec_f,))
    windowed(spec_f)
    products(spec_s, False)
    outputs(0, True)
    products(spec_u, True)
    outputs(1, False)
    early, late = order[:n // 2], order[n // 2:]
    give_back(1, early)

    gather((s1,), (s1_rs,), (spec_s,))
    products(spec_s, False)
    outputs(2, False)

    if nc > 1:
        arrived(zg.at[pl.ds(0, nc - 1)], gz_rs)
    for p in range(n):
        acc = g_send[p, band(mz)].astype(F32)
        for k in range(nc - 1):
            acc += zg[k, p].astype(F32)
        g2_send[p] = acc.astype(BF16)
    for p in peers:
        send(g2_send.at[p], g2_recv.at[me], g2_ss, g2_rs, {"seq": p})
    g2_recv[me] = g2_send[me]
    give_back(1, late)
    give_back(2, order)

    loaded(skip, fq)

    def returned(which):
        for at in range(2):
            group = [flipped(r) for r in offsets[at]]
            if group:
                arrived(c_recv.at[which, pl.ds(0, len(group))], c_rs.at[which, at])
            for q in group + ([me] if at == 0 else []):
                cols = lane(q)
                yield q, cols, skip[:, cols], c_recv[which, q].astype(F32)

    for q, at, gain, value in returned(0):
        mixed = value + gain * s2_send[q].astype(F32)
        gq_o[:, at] = (bg[:, at].astype(F32) * mixed).astype(BF16)
    arrived(g2_recv.at[pl.ds(0, n - 1)], g2_rs)
    for k in range(nc - 2, -1, -1):
        z = zorder[k]
        send(g2_recv.at[pl.ds(z * per, per)], g3.at[mz], g3_ss, g3_rs, {"chan": z})
    for h in range(per):
        g3[mz, h] = g2_recv[mz * per + h]
    arrived(k_recv.at[pl.ds(0, n - 1)], k_rs)
    for q in range(n):
        gs_o[:, q * w:(q + 1) * w] = k_recv[q, 0:1]
    for q, at, gain, value in returned(1):
        through = value + gain * up_send[q].astype(F32)
        gk_o[:, at] = (through * bv[:, at].astype(F32)).astype(BF16)
        gv_o[:, at] = (through * bk[:, at].astype(F32)).astype(BF16)
    for q, at, gain, value in returned(2):
        mixed = value + gain * s1_send[q].astype(F32)
        out_o[:, at] = (fq[:, at].astype(F32) * mixed).astype(BF16)
    if nc > 1:
        arrived(g3.at[pl.ds(0, nc - 1)], g3_rs)
    for z in range(nc):
        for h in range(per):
            gf_o[z * part:(z + 1) * part, h * w:(h + 1) * w] = g3[z, h].astype(F32)

    sent(c_send.at[:, pl.ds(0, n - 1)], in_ss)
    sent(c_send.at[:, pl.ds(0, n - 1)], c_ss)
    sent(rf.at[pl.ds(0, n - 1)], f_ss)
    sent(g2_send.at[pl.ds(0, n - 1)], g2_ss)
    sent(k_recv.at[pl.ds(0, n - 1)], k_ss)
    if nc > 1:
        sent(fz.at[pl.ds(0, (nc - 1) * per)], z_ss)
        sent(zg.at[pl.ds(0, nc - 1)], gz_ss)
        sent(g3.at[pl.ds(0, nc - 1)], g3_ss)


def store_all(*refs):
    count = len(refs) // 2
    near, far, sems = refs[:count], refs[count:2 * count], refs[-1]
    stores = [pltpu.make_async_copy(near[i], far[i], sems.at[i]) for i in range(count)]
    for c in stores:
        c.start()
    for c in stores:
        c.wait()


def fused_device(n, nc, *args):
    fwd_q, filters, skip = args[0], args[7], args[8]
    rows, chan_width = fwd_q.shape
    w = chan_width // n
    per = filters.shape[1] // w
    part = rows // nc
    scale = 1.0 / math.sqrt(rows * n)
    forward, inverse = (jnp.asarray(t, dtype=BF16) for t in block_tables(2 * rows))
    results = (
        *[pltpu.VMEM((rows, chan_width), BF16)] * 4, pltpu.VMEM(filters.shape, F32), pltpu.VMEM((1, chan_width), F32),
    )
    dma = pltpu.SemaphoreType.DMA
    block = (n, rows, w)
    spectrum = (n // 2, 4 * rows, w)
    scratch = [
        *[pltpu.VMEM((rows, chan_width), BF16)] * 7, pltpu.VMEM(filters.shape, F32),
        pltpu.VMEM((1, chan_width), F32), pltpu.VMEM(forward.shape, BF16), pltpu.VMEM(inverse.shape, BF16),
        dma((11,)),
        *[pltpu.VMEM(block, BF16)] * 8,
        *[pltpu.VMEM(spectrum, F32)] * 5,
        pltpu.VMEM((3,) + block, BF16), pltpu.VMEM((3,) + block, BF16),
        pltpu.VMEM(block, BF16), pltpu.VMEM((nc, n, part, w), BF16),
        pltpu.VMEM((n, part, w), BF16), pltpu.VMEM((n, part, w), BF16), pltpu.VMEM((nc, per, part, w), BF16),
        pltpu.VMEM((8, w), F32), pltpu.VMEM((n, 8, w), F32),
        dma, *[dma((2,))] * 3, dma, dma((2,)), dma, dma((nc,)), pltpu.SemaphoreType.REGULAR,
        dma, dma((3, 2)), *[dma] * 8,
    ]
    operands = (*args[:8], skip.reshape(1, chan_width), forward, inverse)
    hbm, vmem = (pl.BlockSpec(memory_space=m) for m in (pltpu.HBM, pltpu.VMEM))
    outs = pl.pallas_call(
        functools.partial(kernel, n, nc, scale),
        out_shape=results,
        in_specs=[hbm] * 11,
        out_specs=(vmem,) * 6,
        scratch_shapes=scratch,
        compiler_params=pltpu.CompilerParams(
            collective_id=0, has_side_effects=True, vmem_limit_bytes=KERNEL_VMEM
        ),
    )(*[pltpu.with_memory_space_constraint(a, pltpu.HBM) for a in operands])
    outs = pl.pallas_call(
        store_all,
        out_shape=tuple(jax.ShapeDtypeStruct(o.shape, o.dtype) for o in outs),
        in_specs=[vmem] * 6,
        out_specs=(hbm,) * 6,
        scratch_shapes=[dma((6,))],
        compiler_params=pltpu.CompilerParams(vmem_limit_bytes=KERNEL_VMEM),
    )(*outs)
    return tuple(outs[:5]) + (outs[5].reshape(chan_width),)


def routed(*args):
    n, nc = lax.axis_size("seq"), lax.axis_size("chan")
    rows, chan_width = args[0].shape
    filter_width = args[7].shape[1]
    fits = chan_width % (n * LANES) == 0 and rows % (16 * nc) == 0 and rows % 32 == 0
    fits = fits and n > 1 and n & (n - 1) == 0 and nc <= REACH + 2
    if fits and filter_width * nc == chan_width and filter_width % (chan_width // n) == 0:
        return fused_device(n, nc, *args)
    return per_device(*args)


def solution(mesh):
    return jax.shard_map(
        routed,
        mesh=mesh,
        in_specs=(
            P("seq", "chan"),
            P("seq", "chan"),
            P("seq", "chan"),
            P("seq", "chan"),
            P("seq", "chan"),
            P("seq", "chan"),
            P("seq", "chan"),
            P("seq", "chan"),
            P("chan"),
        ),
        out_specs=(
            P("seq", "chan"),
            P("seq", "chan"),
            P("seq", "chan"),
            P("seq", "chan"),
            P("seq", "chan"),
            P("chan"),
        ),
        check_vma=False,
    )
```

```python
import functools
import math

import jax
import jax.numpy as jnp
import numpy as np
from jax import lax
from jax.experimental import pallas as pl
from jax.experimental.pallas import tpu as pltpu
from jax.sharding import PartitionSpec as P

HIGHEST = lax.Precision.HIGHEST
LANES = 128
MESH = pl.DeviceIdType.MESH
BF16 = jnp.bfloat16
F32 = jnp.float32
KERNEL_VMEM = 32 * 2**20


def index_ramp(total):
    return jnp.arange(total, dtype=jnp.int32)


def widened(values):
    return values.astype(jnp.float32)


def angles(out_index, in_index, period, sign):
    phase_steps = out_index[:, None] * in_index[None, :] % period
    phase = phase_steps.astype(jnp.float32) * (sign * 2.0 * math.pi / period)
    return (jnp.cos(phase), jnp.sin(phase))


def times_table(left, right):
    return (left[0] * right[0] - left[1] * right[1], left[0] * right[1] + left[1] * right[0])


def block_table(pair):
    cosine, sine_part = pair
    return jnp.stack([jnp.stack([cosine, -sine_part]), jnp.stack([sine_part, cosine])])


def product_of(left, right):
    return jnp.stack(
        [left[0] * right[0] - left[1] * right[1], left[0] * right[1] + left[1] * right[0]]
    )


def conj_product(left, right):
    return jnp.stack(
        [left[0] * right[0] + left[1] * right[1], left[0] * right[1] - left[1] * right[0]]
    )


def joined(left, right):
    return jnp.concatenate([left, right], axis=-1)


def factor(total):
    chosen = 1
    for candidate in range(1, total + 1):
        if candidate * candidate <= total and total % candidate == 0:
            chosen = candidate
    return chosen


def leading_section(values, seq_size):
    cosine, sine_part = angles(index_ramp(2 * seq_size), index_ramp(seq_size), 2 * seq_size, -1.0)
    table = jnp.stack([cosine, sine_part])
    return jnp.einsum("rkp,pmc->rkmc", table, values, precision=HIGHEST)


def trailing_section(values, seq_size, period):
    cosine, sine_part = angles(index_ramp(seq_size), index_ramp(2 * seq_size), 2 * seq_size, 1.0)
    table = jnp.stack([cosine, -sine_part]) * (1.0 / period)
    return jnp.einsum("rpk,rkmc->pmc", table, values, precision=HIGHEST)


def inner_forward(values, freq_keys, period):
    lead_size, row_count, chan_count = values.shape[1:]
    outer_size = factor(row_count)
    inner_size = row_count // outer_size
    values = values.reshape(2, lead_size, outer_size, inner_size, chan_count)
    first_twiddle = angles(freq_keys, index_ramp(row_count), period, -1.0)
    first_twiddle = tuple(
        (part.reshape(lead_size, outer_size, inner_size) for part in first_twiddle)
    )
    outer_dft = angles(index_ramp(outer_size), index_ramp(outer_size), outer_size, -1.0)
    outer_table = times_table(
        tuple((part[None, :, :, None] for part in outer_dft)),
        tuple((part[:, None, :, :] for part in first_twiddle)),
    )
    values = jnp.einsum("rsjxab,sjabc->rjxbc", block_table(outer_table), values, precision=HIGHEST)
    second_twiddle = angles(index_ramp(outer_size), index_ramp(inner_size), row_count, -1.0)
    inner_dft = angles(index_ramp(inner_size), index_ramp(inner_size), inner_size, -1.0)
    inner_table = times_table(
        tuple((part[None, :, :] for part in inner_dft)),
        tuple((part[:, None, :] for part in second_twiddle)),
    )
    return jnp.einsum("rsxyb,sjxbc->rjxyc", block_table(inner_table), values, precision=HIGHEST)


def inner_inverse(values, freq_keys, period):
    lead_size, outer_size, inner_size, chan_count = values.shape[1:]
    row_count = outer_size * inner_size
    second_twiddle = angles(index_ramp(outer_size), index_ramp(inner_size), row_count, 1.0)
    inner_dft = angles(index_ramp(inner_size), index_ramp(inner_size), inner_size, 1.0)
    inner_table = times_table(
        tuple((part[:, :, None] for part in second_twiddle)),
        tuple((part[None, :, :] for part in inner_dft)),
    )
    values = jnp.einsum("rsxby,sjxyc->rjxbc", block_table(inner_table), values, precision=HIGHEST)
    first_twiddle = angles(freq_keys, index_ramp(row_count), period, 1.0)
    first_twiddle = tuple(
        (part.reshape(lead_size, outer_size, inner_size) for part in first_twiddle)
    )
    outer_dft = angles(index_ramp(outer_size), index_ramp(outer_size), outer_size, 1.0)
    outer_table = times_table(
        tuple((part[:, :, :, None] for part in first_twiddle)),
        tuple((part[None, :, None, :] for part in outer_dft)),
    )
    values = jnp.einsum("rsjabx,sjxbc->rjabc", block_table(outer_table), values, precision=HIGHEST)
    return values.reshape(2, lead_size, row_count, chan_count)


def forward_local(signal_part, seq_size):
    seq_length, chan_count = signal_part.shape
    row_count = seq_length // seq_size
    values = leading_section(signal_part.reshape(seq_size, row_count, chan_count), seq_size)
    return inner_forward(values, index_ramp(2 * seq_size), 2 * seq_length)


def inverse_local(values, seq_size):
    lead_size, outer_size, inner_size, chan_count = values.shape[1:]
    row_count = outer_size * inner_size
    period = 2 * seq_size * row_count
    values = inner_inverse(values, index_ramp(2 * seq_size), period)
    return trailing_section(values, seq_size, period).reshape(seq_size * row_count, chan_count)


def filter_times_pair(spec_filter, spec_pair):
    shape_pair = spec_pair.shape
    width = spec_filter.shape[-1]
    pair_view = spec_pair.reshape(shape_pair[:-1] + (2, width))
    filter_view = spec_filter[..., None, :]
    return product_of(filter_view, pair_view).reshape(shape_pair)


def per_device(fwd_q, fwd_k, fwd_v, bwd_q, bwd_k, bwd_v, bwd_grad, filters, skip):
    row_count, chan_width = fwd_q.shape
    seq_size = lax.axis_size("seq")
    grad_scale = 1.0 / math.sqrt(row_count * seq_size)
    source = (widened(fwd_k) * widened(fwd_v)).astype(jnp.bfloat16)
    second_source = (widened(bwd_k) * widened(bwd_v)).astype(jnp.bfloat16)
    upstream = (widened(bwd_grad) * widened(bwd_q)).astype(jnp.bfloat16)
    skip_gain = widened(skip)
    filters_all = lax.all_gather(filters, "chan", axis=1, tiled=True)
    narrow = chan_width // seq_size
    local_first, local_second = (
        lax.all_to_all(source, "seq", split_axis=1, concat_axis=0, tiled=True),
        lax.all_to_all(second_source, "seq", split_axis=1, concat_axis=0, tiled=True),
    )
    local_filter = lax.all_to_all(filters_all, "seq", split_axis=1, concat_axis=0, tiled=True)
    local_up = lax.all_to_all(upstream, "seq", split_axis=1, concat_axis=0, tiled=True)
    spec_sources = forward_local(
        widened(jnp.concatenate([local_first, local_second], axis=1)), seq_size
    )
    spec_filter = forward_local(local_filter, seq_size)
    conv_local = inverse_local(filter_times_pair(spec_filter, spec_sources), seq_size)
    conv_first, conv_second = (
        lax.all_to_all(conv_local[:, :narrow], "seq", split_axis=0, concat_axis=1, tiled=True),
        lax.all_to_all(conv_local[:, narrow:], "seq", split_axis=0, concat_axis=1, tiled=True),
    )
    spec_up = forward_local(widened(local_up), seq_size)
    spec_second = spec_sources[..., narrow:]
    back_local = inverse_local(
        joined(conj_product(spec_filter, spec_up), conj_product(spec_second, spec_up)), seq_size
    )
    through_conv, filter_terms = (
        lax.all_to_all(back_local[:, :narrow], "seq", split_axis=0, concat_axis=1, tiled=True),
        lax.all_to_all(
            back_local[:, narrow:] * grad_scale, "seq", split_axis=0, concat_axis=1, tiled=True
        ),
    )
    grad_filter = lax.psum_scatter(filter_terms, "chan", scatter_dimension=1, tiled=True)
    source_wide = widened(source)
    second_wide = widened(second_source)
    upstream_wide = widened(upstream)
    mixed = conv_first + skip_gain * source_wide
    output = (widened(fwd_q) * mixed).astype(jnp.bfloat16)
    mixed_two = conv_second + skip_gain * second_wide
    grad_query = (widened(bwd_grad) * mixed_two).astype(jnp.bfloat16)
    through = through_conv + skip_gain * upstream_wide
    grad_key = (through * widened(bwd_v)).astype(jnp.bfloat16)
    grad_value = (through * widened(bwd_k)).astype(jnp.bfloat16)
    grad_skip = lax.psum(jnp.sum(upstream_wide * second_wide, axis=0) * grad_scale, "seq")
    return (output, grad_query, grad_key, grad_value, grad_filter, grad_skip)


def block_tables(rows):
    freq = 2 * np.arange(rows)[:, None] + 1
    phase = (freq * np.arange(rows)[None, :] % (4 * rows)) * (np.pi / (2 * rows))
    forward = np.concatenate([np.cos(phase), -np.sin(phase)], axis=0)
    inverse = np.concatenate([np.cos(phase), -np.sin(phase)], axis=0).T / rows
    return forward.astype(np.float32), inverse.astype(np.float32)


REACH = 2


def kernel(
    n, nc, scale,
    fq_h, fk_h, fv_h, bq_h, bk_h, bv_h, bg_h, filt_h, skip_h, fwd_h, inv_h,
    out_o, gq_o, gk_o, gv_o, gf_o, gs_o,
    fq, fk, fv, bq, bk, bv, bg, filt, skip, fwd_t, inv_t, in_sem,
    s2_send, up_send, s1_send, f_send, fz, s2, up, s1, rf, spec_s, spec_u, spec_f, spec_w, spec_v, prod,
    c_send, c_recv, g_send, zg, g2_send, g2_recv, k_send, k_recv,
    in_ss, s2_rs, up_rs, s1_rs, f_ss, f_rs, z_ss, z_rs, credit, c_ss, c_rs,
    gz_ss, gz_rs, g2_ss, g2_rs, k_ss, k_rs,
):
    rows, chan_width = fq.shape
    w = chan_width // n
    per = filt.shape[1] // w
    part, unit = rows // nc, w // nc
    me = lax.axis_index("seq")
    mz = lax.axis_index("chan")

    def flipped(r):
        at, bit = me, 1
        while bit < n:
            if r & bit:
                at = at + bit * (1 - 2 * lax.rem(me // bit, 2))
            bit *= 2
        return at

    order = sorted(range(1, n), key=lambda r: (r & 1, -r))
    peers = [flipped(r) for r in order]
    paired = list(zip(order, peers))
    upward = 2 * mz < nc
    zorder = []
    for k in range(nc - 1):
        j = nc - 1 - k
        zorder.append(jnp.where(upward, jnp.where(mz <= k, k + 1, k), jnp.where(mz >= j, j - 1, j)))

    def near(z):
        return (z - mz <= REACH) & (mz - z <= REACH)

    slot = lax.broadcasted_iota(jnp.int32, (part, w), 1) // unit
    own_slot = lax.rem(slot + nc - lax.rem(me, nc), nc)

    def turned(x, k):
        return pltpu.roll(x, (k % nc) * unit, 1) if k % nc else x

    def pick(choices, shift=None):
        out = choices[0]
        for k in range(1, nc):
            at = own_slot == k if shift is None else slot == (k + shift) % nc
            out = jnp.where(at, choices[k], out)
        return out

    def copy(src, dst, ss, rs, to):
        return pltpu.make_async_remote_copy(
            src_ref=src, dst_ref=dst, send_sem=ss, recv_sem=rs, device_id=to, device_id_type=MESH
        )

    def send(src, dst, ss, rs, to):
        copy(src, dst, ss, rs, to).start()

    def arrived(buf, rs):
        copy(buf, buf, rs, rs, {"seq": peers[0]}).wait_recv()

    def sent(buf, ss):
        copy(buf, buf, ss, ss, {"seq": peers[0]}).wait_send()

    span, count = 2 * rows, n // 2
    near_side = 2 * (count // 2)

    def side(r):
        return 1 if r >= near_side else 0

    offsets = (range(1, near_side), range(max(near_side, 1), n))

    loads = {}
    order_in = ((bk_h, bk), (bv_h, bv), (filt_h, filt), (bg_h, bg), (bq_h, bq), (fk_h, fk), (fv_h, fv))
    for at, (far, dst) in enumerate(order_in + ((fwd_h, fwd_t), (inv_h, inv_t), (skip_h, skip), (fq_h, fq))):
        loads[id(dst)] = pltpu.make_async_copy(far, dst, in_sem.at[at])
        loads[id(dst)].start()

    def loaded(*refs):
        for ref in refs:
            loads[id(ref)].wait()

    barrier = pltpu.get_barrier_semaphore()
    for p in peers:
        pl.semaphore_signal(barrier, inc=1, device_id={"seq": p}, device_id_type=MESH)
    greeted = n - 1
    for z in zorder:
        greeted = greeted + near(z).astype(jnp.int32)

        @pl.when(near(z))
        def _(z=z):
            pl.semaphore_signal(barrier, inc=1, device_id={"chan": z}, device_id_type=MESH)

    chips = [flipped(r) // 2 for r in range(n - 2, 0, -2)] + [me // 2]

    def transform(dst, c, src):
        block = jnp.concatenate([src[2 * c], src[2 * c + 1]], axis=0)
        dst[c] = jnp.dot(fwd_t[...], block, preferred_element_type=F32)

    def gated(dst, left, right):
        for k in range(nc):
            band_rows = slice(k * part, (k + 1) * part)
            for hi in range(per):
                pieces = []
                for o in range(nc):
                    cols = slice((o * per + hi) * w, (o * per + hi + 1) * w)
                    value = left[band_rows, cols].astype(F32) * right[band_rows, cols].astype(F32)
                    pieces.append(turned(value, o))
                for j in range(nc):
                    dst[hi * nc + j, band_rows] = pick(pieces, j).astype(BF16)

    loaded(bk, bv)
    gated(s2_send, bk, bv)
    loaded(filt)
    for hi in range(per):
        cols = slice(hi * w, (hi + 1) * w)
        pieces = [turned(filt[k * part:(k + 1) * part, cols], k) for k in range(nc)]
        for j in range(nc):
            f_send[hi * nc + j] = pick(pieces, j).astype(BF16)
    pl.semaphore_wait(barrier, greeted)

    for r, p in paired:
        send(f_send.at[p], fz.at[mz, me], f_ss, f_rs.at[r // 2], {"seq": p})
    fz[mz, me] = f_send[me]

    distant = ~near(zorder[-1]) if nc > 1 else None
    if nc > 1:
        o = zorder[-1]
        other = jnp.where(o > mz, mz - 1, mz + 1)
        vouch = ((o - mz == REACH) | (mz - o == REACH)) & (other >= 0) & (other < nc)

        @pl.when(vouch)
        def _():
            pl.semaphore_signal(credit, inc=1, device_id={"chan": o}, device_id_type=MESH)

    def scatter(src, dst, ss, rs):
        for r, p in paired:
            send(src.at[p], dst.at[me], ss, rs.at[side(r)], {"seq": p})
        dst[me] = src[me]

    scatter(s2_send, s2, in_ss, s2_rs)
    loaded(bg, bq)
    gated(up_send, bg, bq)
    scatter(up_send, up, in_ss, up_rs)
    loaded(fk, fv)
    gated(s1_send, fk, fv)

    for i, c in enumerate(chips[::-1]):
        fresh = fz.at[mz, pl.ds(2 * c, 2)]
        arrived(fresh if i else fz.at[mz, pl.ds(0, 1)], f_rs.at[i])
        if nc > 1 and i == 0:
            @pl.when(distant)
            def _():
                pl.semaphore_wait(credit, 1)
        for k in range(nc - 2, -1, -1):
            send(fresh, fresh, z_ss, z_rs.at[mz], {"chan": zorder[k]})
    loaded(fwd_t, inv_t)

    sign = 1.0 - 2.0 * lax.rem(lax.broadcasted_iota(jnp.int32, (span, w), 0), 2).astype(F32)

    def windowed(dst, src):
        dst[0] = src[0]
        for d in range(1, count):
            dst[d, :span] = src[d, :span] - sign * src[d - 1, span:]
            dst[d, span:] = src[d, span:] + sign * src[d - 1, :span]

    def products(win, src, corr):
        def tile(k, carry):
            re_at = pl.ds(pl.multiple_of(k * 16, 16), 16)
            im_at = pl.ds(pl.multiple_of(span + k * 16, 16), 16)
            ar = [win[d, re_at] for d in range(count)]
            ai = [win[d, im_at] for d in range(count)]
            xr = [src[d, re_at] for d in range(count)]
            xi = [src[d, im_at] for d in range(count)]
            for b in range(count):
                terms = [(c - b, c) for c in range(b, count)] if corr else [(b - c, c) for c in range(b + 1)]
                re, im = None, None
                for d, c in terms:
                    if corr:
                        tr = ar[d] * xr[c] + ai[d] * xi[c]
                        ti = ar[d] * xi[c] - ai[d] * xr[c]
                    else:
                        tr = ar[d] * xr[c] - ai[d] * xi[c]
                        ti = ar[d] * xi[c] + ai[d] * xr[c]
                    re = tr if re is None else re + tr
                    im = ti if im is None else im + ti
                prod[b, re_at] = re
                prod[b, im_at] = im
            return carry

        lax.fori_loop(0, span // 16, tile, 0)

    def inverse(b):
        return jnp.dot(inv_t[...], prod[b].astype(BF16), preferred_element_type=F32)

    def give_back(which, group):
        for r in group:
            p = flipped(r)
            send(c_send.at[which, p], c_recv.at[which, me], c_ss, c_rs.at[which, side(r)], {"seq": p})

    def halves(dst, c, value):
        dst[2 * c] = value[:rows].astype(BF16)
        dst[2 * c + 1] = value[rows:].astype(BF16)

    def batches(items):
        return [items[:len(items) // 2], items[len(items) // 2:]]

    def outputs(which, now):
        for group in batches(list(range(count))):
            for i in group:
                halves(c_send.at[which], chips[i], inverse(chips[i]))
            if now:
                give_back(which, [r for i in group for r in (n - 2 - 2 * i, n - 1 - 2 * i) if r])
        c_recv[which, me] = c_send[which, me]

    def gather(buf, sems, spec):
        for at, group in enumerate(batches(list(range(count))[::-1])):
            if len(offsets[at]):
                arrived(buf.at[pl.ds(0, len(offsets[at]))], sems.at[at])
            for i in group:
                transform(spec, chips[i], buf)

    gather(s2, s2_rs, spec_s)
    scatter(s1_send, s1, in_ss, s1_rs)
    gather(up, up_rs, spec_u)
    windowed(spec_v, spec_s)
    products(spec_v, spec_u, True)
    for b in range(count):
        value = inverse(b) * scale
        for h in range(2):
            bands = [value[h * rows + k * part:h * rows + (k + 1) * part] for k in range(nc)]
            for o in range(nc):
                g_send[o, 2 * b + h] = pick([turned(bands[k], k - o) for k in range(nc)]).astype(BF16)

    for k in range(nc - 2, -1, -1):
        z = zorder[k]
        send(g_send.at[z], zg.at[jnp.where(mz > z, mz - 1, mz)], gz_ss, gz_rs, {"chan": z})

    for z in zorder:
        arrived(fz.at[z], z_rs.at[z])
    for q in range(n):
        pieces = [fz[o, q].astype(F32) for o in range(nc)]
        for k in range(nc):
            rf[q, k * part:(k + 1) * part] = pick([turned(pieces[o], o - k) for o in range(nc)]).astype(BF16)
    for c in range(count):
        transform(spec_f, c, rf)
    windowed(spec_w, spec_f)
    products(spec_w, spec_s, False)
    outputs(0, True)

    products(spec_w, spec_u, True)
    outputs(1, True)

    total = jnp.zeros((1, w), F32)
    for q in range(n):
        total += jnp.sum(s2[q].astype(F32) * up[q].astype(F32), axis=0, keepdims=True)
    k_send[...] = jnp.broadcast_to(total * scale, k_send.shape)
    for p in peers:
        send(k_send, k_recv.at[me], k_ss, k_rs, {"seq": p})
    k_recv[me] = k_send[...]

    gather(s1, s1_rs, spec_s)
    products(spec_w, spec_s, False)
    outputs(2, True)

    if nc > 1:
        arrived(zg.at[pl.ds(0, nc - 1)], gz_rs)
    for p in range(n):
        acc = g_send[mz, p].astype(F32)
        for k in range(nc - 1):
            acc += zg[k, p].astype(F32)
        g2_send[p] = acc.astype(BF16)
    for p in peers:
        send(g2_send.at[p], g2_recv.at[me], g2_ss, g2_rs, {"seq": p})
    g2_recv[me] = g2_send[me]

    loaded(skip, fq)

    def returned(which):
        for at in range(2):
            if len(offsets[at]):
                arrived(c_recv.at[which, pl.ds(0, len(offsets[at]))], c_rs.at[which, at])
        for k in range(nc):
            at = slice(k * part, (k + 1) * part)
            for hi in range(per):
                values = [c_recv[which, hi * nc + j, at].astype(F32) for j in range(nc)]
                for o in range(nc):
                    cols = slice((o * per + hi) * w, (o * per + hi + 1) * w)
                    yield (at, cols), skip[:, cols], turned(pick(values, o), -o)

    def product(left, right, at):
        return (left[at].astype(F32) * right[at].astype(F32)).astype(BF16).astype(F32)

    for at, gain, value in returned(0):
        mixed = value + gain * product(bk, bv, at)
        gq_o[at] = (bg[at].astype(F32) * mixed).astype(BF16)
    arrived(k_recv.at[pl.ds(0, n - 1)], k_rs)
    sums = k_recv[...]
    for hi in range(per):
        for o in range(nc):
            cols = slice((o * per + hi) * w, (o * per + hi + 1) * w)
            value = sums[hi * nc]
            for j in range(1, nc):
                value = jnp.where(slot[:8] == (o + j) % nc, sums[hi * nc + j], value)
            gs_o[:, cols] = turned(value, -o)[:1]
    for at, gain, value in returned(1):
        through = value + gain * product(bg, bq, at)
        gk_o[at] = (through * bv[at].astype(F32)).astype(BF16)
        gv_o[at] = (through * bk[at].astype(F32)).astype(BF16)
    for at, gain, value in returned(2):
        mixed = value + gain * product(fk, fv, at)
        out_o[at] = (fq[at].astype(F32) * mixed).astype(BF16)

    arrived(g2_recv.at[pl.ds(0, n - 1)], g2_rs)
    for k in range(nc):
        for hi in range(per):
            value = pick([g2_recv[hi * nc + j].astype(F32) for j in range(nc)], k)
            gf_o[k * part:(k + 1) * part, hi * w:(hi + 1) * w] = turned(value, -k)

    sent(c_send.at[:, pl.ds(0, n - 1)], in_ss)
    sent(c_send.at[:, pl.ds(0, n - 1)], c_ss)
    sent(f_send.at[pl.ds(0, n - 1)], f_ss)
    sent(g2_send.at[pl.ds(0, n - 1)], g2_ss)
    sent(k_recv.at[pl.ds(0, n - 1)], k_ss)
    if nc > 1:
        sent(fz.at[pl.ds(0, nc - 1)], z_ss)
        sent(zg.at[pl.ds(0, nc - 1)], gz_ss)


def store_all(*refs):
    count = len(refs) // 2
    near, far, sems = refs[:count], refs[count:2 * count], refs[-1]
    stores = [pltpu.make_async_copy(near[i], far[i], sems.at[i]) for i in range(count)]
    for c in stores:
        c.start()
    for c in stores:
        c.wait()


def fused_device(n, nc, *args):
    fwd_q, filters, skip = args[0], args[7], args[8]
    rows, chan_width = fwd_q.shape
    w = chan_width // n
    per = filters.shape[1] // w
    part = rows // nc
    scale = 1.0 / math.sqrt(rows * n)
    forward, inverse = (jnp.asarray(t, dtype=BF16) for t in block_tables(2 * rows))
    results = (
        *[pltpu.VMEM((rows, chan_width), BF16)] * 4, pltpu.VMEM(filters.shape, F32), pltpu.VMEM((1, chan_width), F32),
    )
    dma = pltpu.SemaphoreType.DMA
    block, bands = (n, rows, w), (n, part, w)
    spectrum = (n // 2, 4 * rows, w)
    scratch = [
        *[pltpu.VMEM((rows, chan_width), BF16)] * 7, pltpu.VMEM(filters.shape, F32),
        pltpu.VMEM((1, chan_width), F32), pltpu.VMEM(forward.shape, BF16), pltpu.VMEM(inverse.shape, BF16),
        dma((11,)),
        *[pltpu.VMEM(block, BF16)] * 3, pltpu.VMEM(bands, BF16), pltpu.VMEM((nc,) + bands, BF16),
        *[pltpu.VMEM(block, BF16)] * 4,
        *[pltpu.VMEM(spectrum, F32)] * 6,
        pltpu.VMEM((3,) + block, BF16), pltpu.VMEM((3,) + block, BF16),
        *[pltpu.VMEM((nc,) + bands, BF16)] * 2, *[pltpu.VMEM(bands, BF16)] * 2,
        pltpu.VMEM((8, w), F32), pltpu.VMEM((n, 8, w), F32),
        dma, *[dma((2,))] * 3, dma, dma((n // 2,)), dma, dma((nc,)), pltpu.SemaphoreType.REGULAR,
        dma, dma((3, 2)), *[dma] * 6,
    ]
    operands = (*args[:8], skip.reshape(1, chan_width), forward, inverse)
    hbm, vmem = (pl.BlockSpec(memory_space=m) for m in (pltpu.HBM, pltpu.VMEM))
    outs = pl.pallas_call(
        functools.partial(kernel, n, nc, scale),
        out_shape=results,
        in_specs=[hbm] * 11,
        out_specs=(vmem,) * 6,
        scratch_shapes=scratch,
        compiler_params=pltpu.CompilerParams(
            collective_id=0, has_side_effects=True, vmem_limit_bytes=KERNEL_VMEM
        ),
    )(*[pltpu.with_memory_space_constraint(a, pltpu.HBM) for a in operands])
    outs = pl.pallas_call(
        store_all,
        out_shape=tuple(jax.ShapeDtypeStruct(o.shape, o.dtype) for o in outs),
        in_specs=[vmem] * 6,
        out_specs=(hbm,) * 6,
        scratch_shapes=[dma((6,))],
        compiler_params=pltpu.CompilerParams(vmem_limit_bytes=KERNEL_VMEM),
    )(*outs)
    return tuple(outs[:5]) + (outs[5].reshape(chan_width),)


def routed(*args):
    n, nc = lax.axis_size("seq"), lax.axis_size("chan")
    rows, chan_width = args[0].shape
    filter_width = args[7].shape[1]
    fits = chan_width % (n * LANES) == 0 and rows % (16 * nc) == 0 and rows % 32 == 0
    fits = fits and n % nc == 0 and n > 1 and n & (n - 1) == 0 and nc <= REACH + 2
    if fits and filter_width * nc == chan_width and filter_width % (chan_width // n) == 0:
        return fused_device(n, nc, *args)
    return per_device(*args)


def solution(mesh):
    return jax.shard_map(
        routed,
        mesh=mesh,
        in_specs=(
            P("seq", "chan"),
            P("seq", "chan"),
            P("seq", "chan"),
            P("seq", "chan"),
            P("seq", "chan"),
            P("seq", "chan"),
            P("seq", "chan"),
            P("seq", "chan"),
            P("chan"),
        ),
        out_specs=(
            P("seq", "chan"),
            P("seq", "chan"),
            P("seq", "chan"),
            P("seq", "chan"),
            P("seq", "chan"),
            P("chan"),
        ),
        check_vma=False,
    )
```

```python
import functools
import math

import jax
import jax.numpy as jnp
import numpy as np
from jax import lax
from jax.experimental import pallas as pl
from jax.experimental.pallas import tpu as pltpu
from jax.sharding import PartitionSpec as P

HIGHEST = lax.Precision.HIGHEST
LANES = 128
MESH = pl.DeviceIdType.MESH
BF16 = jnp.bfloat16
F32 = jnp.float32
KERNEL_VMEM = 32 * 2**20


def index_ramp(total):
    return jnp.arange(total, dtype=jnp.int32)


def widened(values):
    return values.astype(jnp.float32)


def angles(out_index, in_index, period, sign):
    phase_steps = out_index[:, None] * in_index[None, :] % period
    phase = phase_steps.astype(jnp.float32) * (sign * 2.0 * math.pi / period)
    return (jnp.cos(phase), jnp.sin(phase))


def times_table(left, right):
    return (left[0] * right[0] - left[1] * right[1], left[0] * right[1] + left[1] * right[0])


def block_table(pair):
    cosine, sine_part = pair
    return jnp.stack([jnp.stack([cosine, -sine_part]), jnp.stack([sine_part, cosine])])


def product_of(left, right):
    return jnp.stack(
        [left[0] * right[0] - left[1] * right[1], left[0] * right[1] + left[1] * right[0]]
    )


def conj_product(left, right):
    return jnp.stack(
        [left[0] * right[0] + left[1] * right[1], left[0] * right[1] - left[1] * right[0]]
    )


def joined(left, right):
    return jnp.concatenate([left, right], axis=-1)


def factor(total):
    chosen = 1
    for candidate in range(1, total + 1):
        if candidate * candidate <= total and total % candidate == 0:
            chosen = candidate
    return chosen


def leading_section(values, seq_size):
    cosine, sine_part = angles(index_ramp(2 * seq_size), index_ramp(seq_size), 2 * seq_size, -1.0)
    table = jnp.stack([cosine, sine_part])
    return jnp.einsum("rkp,pmc->rkmc", table, values, precision=HIGHEST)


def trailing_section(values, seq_size, period):
    cosine, sine_part = angles(index_ramp(seq_size), index_ramp(2 * seq_size), 2 * seq_size, 1.0)
    table = jnp.stack([cosine, -sine_part]) * (1.0 / period)
    return jnp.einsum("rpk,rkmc->pmc", table, values, precision=HIGHEST)


def inner_forward(values, freq_keys, period):
    lead_size, row_count, chan_count = values.shape[1:]
    outer_size = factor(row_count)
    inner_size = row_count // outer_size
    values = values.reshape(2, lead_size, outer_size, inner_size, chan_count)
    first_twiddle = angles(freq_keys, index_ramp(row_count), period, -1.0)
    first_twiddle = tuple(
        (part.reshape(lead_size, outer_size, inner_size) for part in first_twiddle)
    )
    outer_dft = angles(index_ramp(outer_size), index_ramp(outer_size), outer_size, -1.0)
    outer_table = times_table(
        tuple((part[None, :, :, None] for part in outer_dft)),
        tuple((part[:, None, :, :] for part in first_twiddle)),
    )
    values = jnp.einsum("rsjxab,sjabc->rjxbc", block_table(outer_table), values, precision=HIGHEST)
    second_twiddle = angles(index_ramp(outer_size), index_ramp(inner_size), row_count, -1.0)
    inner_dft = angles(index_ramp(inner_size), index_ramp(inner_size), inner_size, -1.0)
    inner_table = times_table(
        tuple((part[None, :, :] for part in inner_dft)),
        tuple((part[:, None, :] for part in second_twiddle)),
    )
    return jnp.einsum("rsxyb,sjxbc->rjxyc", block_table(inner_table), values, precision=HIGHEST)


def inner_inverse(values, freq_keys, period):
    lead_size, outer_size, inner_size, chan_count = values.shape[1:]
    row_count = outer_size * inner_size
    second_twiddle = angles(index_ramp(outer_size), index_ramp(inner_size), row_count, 1.0)
    inner_dft = angles(index_ramp(inner_size), index_ramp(inner_size), inner_size, 1.0)
    inner_table = times_table(
        tuple((part[:, :, None] for part in second_twiddle)),
        tuple((part[None, :, :] for part in inner_dft)),
    )
    values = jnp.einsum("rsxby,sjxyc->rjxbc", block_table(inner_table), values, precision=HIGHEST)
    first_twiddle = angles(freq_keys, index_ramp(row_count), period, 1.0)
    first_twiddle = tuple(
        (part.reshape(lead_size, outer_size, inner_size) for part in first_twiddle)
    )
    outer_dft = angles(index_ramp(outer_size), index_ramp(outer_size), outer_size, 1.0)
    outer_table = times_table(
        tuple((part[:, :, :, None] for part in first_twiddle)),
        tuple((part[None, :, None, :] for part in outer_dft)),
    )
    values = jnp.einsum("rsjabx,sjxbc->rjabc", block_table(outer_table), values, precision=HIGHEST)
    return values.reshape(2, lead_size, row_count, chan_count)


def forward_local(signal_part, seq_size):
    seq_length, chan_count = signal_part.shape
    row_count = seq_length // seq_size
    values = leading_section(signal_part.reshape(seq_size, row_count, chan_count), seq_size)
    return inner_forward(values, index_ramp(2 * seq_size), 2 * seq_length)


def inverse_local(values, seq_size):
    lead_size, outer_size, inner_size, chan_count = values.shape[1:]
    row_count = outer_size * inner_size
    period = 2 * seq_size * row_count
    values = inner_inverse(values, index_ramp(2 * seq_size), period)
    return trailing_section(values, seq_size, period).reshape(seq_size * row_count, chan_count)


def filter_times_pair(spec_filter, spec_pair):
    shape_pair = spec_pair.shape
    width = spec_filter.shape[-1]
    pair_view = spec_pair.reshape(shape_pair[:-1] + (2, width))
    filter_view = spec_filter[..., None, :]
    return product_of(filter_view, pair_view).reshape(shape_pair)


def per_device(fwd_q, fwd_k, fwd_v, bwd_q, bwd_k, bwd_v, bwd_grad, filters, skip):
    row_count, chan_width = fwd_q.shape
    seq_size = lax.axis_size("seq")
    grad_scale = 1.0 / math.sqrt(row_count * seq_size)
    source = (widened(fwd_k) * widened(fwd_v)).astype(jnp.bfloat16)
    second_source = (widened(bwd_k) * widened(bwd_v)).astype(jnp.bfloat16)
    upstream = (widened(bwd_grad) * widened(bwd_q)).astype(jnp.bfloat16)
    skip_gain = widened(skip)
    filters_all = lax.all_gather(filters, "chan", axis=1, tiled=True)
    narrow = chan_width // seq_size
    local_first, local_second = (
        lax.all_to_all(source, "seq", split_axis=1, concat_axis=0, tiled=True),
        lax.all_to_all(second_source, "seq", split_axis=1, concat_axis=0, tiled=True),
    )
    local_filter = lax.all_to_all(filters_all, "seq", split_axis=1, concat_axis=0, tiled=True)
    local_up = lax.all_to_all(upstream, "seq", split_axis=1, concat_axis=0, tiled=True)
    spec_sources = forward_local(
        widened(jnp.concatenate([local_first, local_second], axis=1)), seq_size
    )
    spec_filter = forward_local(local_filter, seq_size)
    conv_local = inverse_local(filter_times_pair(spec_filter, spec_sources), seq_size)
    conv_first, conv_second = (
        lax.all_to_all(conv_local[:, :narrow], "seq", split_axis=0, concat_axis=1, tiled=True),
        lax.all_to_all(conv_local[:, narrow:], "seq", split_axis=0, concat_axis=1, tiled=True),
    )
    spec_up = forward_local(widened(local_up), seq_size)
    spec_second = spec_sources[..., narrow:]
    back_local = inverse_local(
        joined(conj_product(spec_filter, spec_up), conj_product(spec_second, spec_up)), seq_size
    )
    through_conv, filter_terms = (
        lax.all_to_all(back_local[:, :narrow], "seq", split_axis=0, concat_axis=1, tiled=True),
        lax.all_to_all(
            back_local[:, narrow:] * grad_scale, "seq", split_axis=0, concat_axis=1, tiled=True
        ),
    )
    grad_filter = lax.psum_scatter(filter_terms, "chan", scatter_dimension=1, tiled=True)
    source_wide = widened(source)
    second_wide = widened(second_source)
    upstream_wide = widened(upstream)
    mixed = conv_first + skip_gain * source_wide
    output = (widened(fwd_q) * mixed).astype(jnp.bfloat16)
    mixed_two = conv_second + skip_gain * second_wide
    grad_query = (widened(bwd_grad) * mixed_two).astype(jnp.bfloat16)
    through = through_conv + skip_gain * upstream_wide
    grad_key = (through * widened(bwd_v)).astype(jnp.bfloat16)
    grad_value = (through * widened(bwd_k)).astype(jnp.bfloat16)
    grad_skip = lax.psum(jnp.sum(upstream_wide * second_wide, axis=0) * grad_scale, "seq")
    return (output, grad_query, grad_key, grad_value, grad_filter, grad_skip)


def block_tables(rows):
    freq = 2 * np.arange(rows)[:, None] + 1
    phase = (freq * np.arange(rows)[None, :] % (4 * rows)) * (np.pi / (2 * rows))
    forward = np.concatenate([np.cos(phase), -np.sin(phase)], axis=0)
    inverse = np.concatenate([np.cos(phase), -np.sin(phase)], axis=0).T / rows
    return forward.astype(np.float32), inverse.astype(np.float32)


REACH = 2


def kernel(
    n, nc, scale,
    fq_h, fk_h, fv_h, bq_h, bk_h, bv_h, bg_h, filt_h, skip_h, fwd_h, inv_h,
    out_o, gq_o, gk_o, gv_o, gf_o, gs_o,
    fq, fk, fv, bq, bk, bv, bg, filt, skip, fwd_t, inv_t, in_sem,
    s2_send, up_send, s1_send, f_send, fz, s2, up, s1, rf, spec_s, spec_u, spec_f, spec_w, prod,
    c_send, c_recv, g_send, zg, g2_send, g2_recv, k_send, k_recv,
    in_ss, s2_rs, up_rs, s1_rs, f_ss, f_rs, z_ss, z_rs, credit, c_ss, c_rs,
    gz_ss, gz_rs, g2_ss, g2_rs, k_ss, k_rs,
):
    rows, chan_width = fq.shape
    w = chan_width // n
    per = filt.shape[1] // w
    part, unit = rows // nc, w // nc
    me = lax.axis_index("seq")
    mz = lax.axis_index("chan")

    def flipped(r):
        at, bit = me, 1
        while bit < n:
            if r & bit:
                at = at + bit * (1 - 2 * lax.rem(me // bit, 2))
            bit *= 2
        return at

    order = sorted(range(1, n), key=lambda r: (r & 1, -r))
    peers = [flipped(r) for r in order]
    paired = list(zip(order, peers))
    upward = 2 * mz < nc
    zorder = []
    for k in range(nc - 1):
        j = nc - 1 - k
        zorder.append(jnp.where(upward, jnp.where(mz <= k, k + 1, k), jnp.where(mz >= j, j - 1, j)))

    def near(z):
        return (z - mz <= REACH) & (mz - z <= REACH)

    slot = lax.broadcasted_iota(jnp.int32, (part, w), 1) // unit
    own_slot = lax.rem(slot + nc - lax.rem(me, nc), nc)

    def turned(x, k):
        return pltpu.roll(x, (k % nc) * unit, 1) if k % nc else x

    def pick(choices, shift=None):
        out = choices[0]
        for k in range(1, nc):
            at = own_slot == k if shift is None else slot == (k + shift) % nc
            out = jnp.where(at, choices[k], out)
        return out

    def copy(src, dst, ss, rs, to):
        return pltpu.make_async_remote_copy(
            src_ref=src, dst_ref=dst, send_sem=ss, recv_sem=rs, device_id=to, device_id_type=MESH
        )

    def send(src, dst, ss, rs, to):
        copy(src, dst, ss, rs, to).start()

    def arrived(buf, rs):
        copy(buf, buf, rs, rs, {"seq": peers[0]}).wait_recv()

    def sent(buf, ss):
        copy(buf, buf, ss, ss, {"seq": peers[0]}).wait_send()

    span, count = 2 * rows, n // 2
    parts = [list(range(count))[i:i + 2] for i in range(0, count, 2)]

    def side(r):
        return len(parts) - 1 - (count - 1 - r // 2) // 2

    loads = (
        ((bk_h, bk), (bv_h, bv)), ((filt_h, filt),), ((bg_h, bg), (bq_h, bq)), ((fk_h, fk), (fv_h, fv), (fq_h, fq)),
        ((fwd_h, fwd_t),), ((inv_h, inv_t),), ((skip_h, skip),),
    )
    for at, group in enumerate(loads):
        for far, dst in group:
            pltpu.make_async_copy(far, dst, in_sem.at[at]).start()

    def loaded(*which):
        for at in which:
            whole = loads[at][0][1] if len(loads[at]) == 1 else c_send.at[pl.ds(0, len(loads[at]))]
            pltpu.make_async_copy(whole, whole, in_sem.at[at]).wait()

    barrier = pltpu.get_barrier_semaphore()
    for p in peers:
        pl.semaphore_signal(barrier, inc=1, device_id={"seq": p}, device_id_type=MESH)
    greeted = n - 1
    for z in zorder:
        greeted = greeted + near(z).astype(jnp.int32)

        @pl.when(near(z))
        def _(z=z):
            pl.semaphore_signal(barrier, inc=1, device_id={"chan": z}, device_id_type=MESH)

    chips = [flipped(r) // 2 for r in range(n - 2, 0, -2)] + [me // 2]

    def transform(dst, group, src):
        blocks = [jnp.concatenate([src[2 * c], src[2 * c + 1]], axis=0) for c in group]
        value = jnp.dot(fwd_t[...], jnp.concatenate(blocks, axis=1), preferred_element_type=F32)
        for i, c in enumerate(group):
            dst[c] = value[:, i * w:(i + 1) * w]

    def gated(dst, left, right):
        for k in range(nc):
            band_rows = slice(k * part, (k + 1) * part)
            for hi in range(per):
                pieces = []
                for o in range(nc):
                    cols = slice((o * per + hi) * w, (o * per + hi + 1) * w)
                    value = left[band_rows, cols].astype(F32) * right[band_rows, cols].astype(F32)
                    pieces.append(turned(value, o))
                for j in range(nc):
                    dst[hi * nc + j, band_rows] = pick(pieces, j).astype(BF16)

    loaded(0)
    gated(s2_send, bk, bv)
    loaded(1)
    for hi in range(per):
        cols = slice(hi * w, (hi + 1) * w)
        pieces = [turned(filt[k * part:(k + 1) * part, cols], k) for k in range(nc)]
        for j in range(nc):
            f_send[hi * nc + j] = pick(pieces, j).astype(BF16)
    pl.semaphore_wait(barrier, greeted)

    for r, p in paired:
        send(f_send.at[p], fz.at[mz, me], f_ss, f_rs.at[r // 2], {"seq": p})
    fz[mz, me] = f_send[me]

    distant = ~near(zorder[-1]) if nc > 1 else None
    if nc > 1:
        o = zorder[-1]
        other = jnp.where(o > mz, mz - 1, mz + 1)
        vouch = ((o - mz == REACH) | (mz - o == REACH)) & (other >= 0) & (other < nc)

        @pl.when(vouch)
        def _():
            pl.semaphore_signal(credit, inc=1, device_id={"chan": o}, device_id_type=MESH)

    def scatter(src, dst, ss, rs):
        for r, p in paired:
            send(src.at[p], dst.at[me], ss, rs.at[side(r)], {"seq": p})
        dst[me] = src[me]

    scatter(s2_send, s2, in_ss, s2_rs)
    loaded(2)
    gated(up_send, bg, bq)
    scatter(up_send, up, in_ss, up_rs)
    loaded(3)
    gated(s1_send, fk, fv)

    for i, c in enumerate(chips[::-1]):
        fresh = fz.at[mz, pl.ds(2 * c, 2)]
        arrived(fresh if i else fz.at[mz, pl.ds(0, 1)], f_rs.at[i])
        if nc > 1 and i == 0:
            @pl.when(distant)
            def _():
                pl.semaphore_wait(credit, 1)
        for k in range(nc - 2, -1, -1):
            send(fresh, fresh, z_ss, z_rs, {"chan": zorder[k]})
    loaded(4, 5)

    sign = 1.0 - 2.0 * lax.rem(lax.broadcasted_iota(jnp.int32, (16, w), 0), 2).astype(F32)

    def products(win, src, corr, raw=None):
        def tile(k, carry):
            re_at = pl.ds(pl.multiple_of(k * 16, 16), 16)
            im_at = pl.ds(pl.multiple_of(span + k * 16, 16), 16)
            if raw is None:
                ar = [win[d, re_at] for d in range(count)]
                ai = [win[d, im_at] for d in range(count)]
            else:
                br = [raw[d, re_at] for d in range(count)]
                bi = [raw[d, im_at] for d in range(count)]
                ar = br[:1] + [br[d] - sign * bi[d - 1] for d in range(1, count)]
                ai = bi[:1] + [bi[d] + sign * br[d - 1] for d in range(1, count)]
                for d in range(count if win is not None else 0):
                    win[d, re_at] = ar[d]
                    win[d, im_at] = ai[d]
            xr = [src[d, re_at] for d in range(count)]
            xi = [src[d, im_at] for d in range(count)]
            for b in range(count):
                terms = [(c - b, c) for c in range(b, count)] if corr else [(b - c, c) for c in range(b + 1)]
                re, im = None, None
                for d, c in terms:
                    if corr:
                        tr = ar[d] * xr[c] + ai[d] * xi[c]
                        ti = ar[d] * xi[c] - ai[d] * xr[c]
                    else:
                        tr = ar[d] * xr[c] - ai[d] * xi[c]
                        ti = ar[d] * xi[c] + ai[d] * xr[c]
                    re = tr if re is None else re + tr
                    im = ti if im is None else im + ti
                prod[b, re_at] = re.astype(BF16)
                prod[b, im_at] = im.astype(BF16)
            return carry

        lax.fori_loop(0, span // 16, tile, 0)

    def inverse(group):
        blocks = [prod[c] for c in group]
        value = jnp.dot(inv_t[...], jnp.concatenate(blocks, axis=1), preferred_element_type=F32)
        return [value[:, i * w:(i + 1) * w] for i in range(len(group))]

    def give_back(which, group):
        for r in group:
            p = flipped(r)
            send(c_send.at[which, p], c_recv.at[which, me], c_ss, c_rs.at[which], {"seq": p})

    def halves(dst, c, value):
        dst[2 * c] = value[:rows].astype(BF16)
        dst[2 * c + 1] = value[rows:].astype(BF16)


    def outputs(which, now):
        values = [inverse([chips[i] for i in group]) for group in parts]
        for group, results in zip(parts, values):
            for i, value in zip(group, results):
                halves(c_send.at[which], chips[i], value)
            if now:
                give_back(which, [r for i in group for r in (n - 2 - 2 * i, n - 1 - 2 * i) if r])
        c_recv[which, me] = c_send[which, me]

    def gather(buf, sems, spec):
        for at, group in enumerate(parts[::-1]):
            arrived(buf.at[pl.ds(0, 2 * len(group) - (at == 0))], sems.at[at])
            transform(spec, [chips[i] for i in group], buf)

    gather(s2, s2_rs, spec_s)
    scatter(s1_send, s1, in_ss, s1_rs)
    gather(up, up_rs, spec_u)
    products(None, spec_u, True, spec_s)
    for group in parts:
        for b, value in zip(group, inverse(group)):
            for h in range(2):
                bands = [value[h * rows + k * part:h * rows + (k + 1) * part] * scale for k in range(nc)]
                for o in range(nc):
                    g_send[o, 2 * b + h] = pick([turned(bands[k], k - o) for k in range(nc)]).astype(BF16)

    for k in range(nc - 2, -1, -1):
        z = zorder[k]
        send(g_send.at[z], zg.at[jnp.where(mz > z, mz - 1, mz)], gz_ss, gz_rs, {"chan": z})

    if nc > 1:
        arrived(fz.at[pl.ds(0, nc - 1)], z_rs)
    for q in range(n):
        pieces = [fz[o, q].astype(F32) for o in range(nc)]
        for k in range(nc):
            rf[q, k * part:(k + 1) * part] = pick([turned(pieces[o], o - k) for o in range(nc)]).astype(BF16)
    for group in parts:
        transform(spec_f, group, rf)
    products(spec_w, spec_s, False, spec_f)
    outputs(0, True)

    products(spec_w, spec_u, True)
    outputs(1, True)

    total = jnp.zeros((1, w), F32)
    for q in range(n):
        total += jnp.sum(s2[q].astype(F32) * up[q].astype(F32), axis=0, keepdims=True)
    k_send[...] = total * scale
    for p in peers:
        send(k_send, k_recv.at[me], k_ss, k_rs, {"seq": p})
    k_recv[me] = k_send[...]

    gather(s1, s1_rs, spec_s)
    products(spec_w, spec_s, False)
    outputs(2, True)

    if nc > 1:
        arrived(zg.at[pl.ds(0, nc - 1)], gz_rs)
    for p in range(n):
        acc = g_send[mz, p].astype(F32)
        for k in range(nc - 1):
            acc += zg[k, p].astype(F32)
        g2_send[p] = acc.astype(BF16)
    for p in peers:
        send(g2_send.at[p], g2_recv.at[me], g2_ss, g2_rs, {"seq": p})
    g2_recv[me] = g2_send[me]

    loaded(6)

    def returned(which):
        arrived(c_recv.at[which, pl.ds(0, n - 1)], c_rs.at[which])
        for k in range(nc):
            at = slice(k * part, (k + 1) * part)
            for hi in range(per):
                values = [c_recv[which, hi * nc + j, at].astype(F32) for j in range(nc)]
                for o in range(nc):
                    cols = slice((o * per + hi) * w, (o * per + hi + 1) * w)
                    yield (at, cols), skip[:, cols], turned(pick(values, o), -o)

    def product(left, right, at):
        return (left[at].astype(F32) * right[at].astype(F32)).astype(BF16).astype(F32)

    for at, gain, value in returned(0):
        mixed = value + gain * product(bk, bv, at)
        gq_o[at] = (bg[at].astype(F32) * mixed).astype(BF16)
    arrived(k_recv.at[pl.ds(0, n - 1)], k_rs)
    sums = k_recv[...]
    for hi in range(per):
        for o in range(nc):
            cols = slice((o * per + hi) * w, (o * per + hi + 1) * w)
            value = sums[hi * nc]
            for j in range(1, nc):
                value = jnp.where(slot[:1] == (o + j) % nc, sums[hi * nc + j], value)
            gs_o[:, cols] = turned(value, -o)
    for at, gain, value in returned(1):
        through = value + gain * product(bg, bq, at)
        gk_o[at] = (through * bv[at].astype(F32)).astype(BF16)
        gv_o[at] = (through * bk[at].astype(F32)).astype(BF16)
    for at, gain, value in returned(2):
        mixed = value + gain * product(fk, fv, at)
        out_o[at] = (fq[at].astype(F32) * mixed).astype(BF16)

    arrived(g2_recv.at[pl.ds(0, n - 1)], g2_rs)
    for k in range(nc):
        for hi in range(per):
            value = pick([g2_recv[hi * nc + j].astype(F32) for j in range(nc)], k)
            gf_o[k * part:(k + 1) * part, hi * w:(hi + 1) * w] = turned(value, -k)

    sent(c_send.at[:, pl.ds(0, n - 1)], in_ss)
    sent(c_send.at[:, pl.ds(0, n - 1)], c_ss)
    sent(f_send.at[pl.ds(0, n - 1)], f_ss)
    sent(g2_send.at[pl.ds(0, n - 1)], g2_ss)
    sent(k_recv.at[pl.ds(0, n - 1)], k_ss)
    if nc > 1:
        sent(fz.at[pl.ds(0, nc - 1)], z_ss)
        sent(zg.at[pl.ds(0, nc - 1)], gz_ss)


def store_all(*refs):
    count = len(refs) // 2
    near, far, sems = refs[:count], refs[count:2 * count], refs[-1]
    stores = [pltpu.make_async_copy(near[i], far[i], sems.at[i]) for i in range(count)]
    for c in stores:
        c.start()
    for c in stores:
        c.wait()


def fused_device(n, nc, *args):
    fwd_q, filters, skip = args[0], args[7], args[8]
    rows, chan_width = fwd_q.shape
    w = chan_width // n
    per = filters.shape[1] // w
    part = rows // nc
    scale = 1.0 / math.sqrt(rows * n)
    forward, inverse = (jnp.asarray(t, dtype=BF16) for t in block_tables(2 * rows))
    results = (
        *[pltpu.VMEM((rows, chan_width), BF16)] * 4, pltpu.VMEM(filters.shape, F32), pltpu.VMEM((1, chan_width), F32),
    )
    dma = pltpu.SemaphoreType.DMA
    block, bands = (n, rows, w), (n, part, w)
    spectrum = (n // 2, 4 * rows, w)
    scratch = [
        *[pltpu.VMEM((rows, chan_width), BF16)] * 7, pltpu.VMEM(filters.shape, F32),
        pltpu.VMEM((1, chan_width), F32), pltpu.VMEM(forward.shape, BF16), pltpu.VMEM(inverse.shape, BF16),
        dma((7,)),
        *[pltpu.VMEM(block, BF16)] * 3, pltpu.VMEM(bands, BF16), pltpu.VMEM((nc,) + bands, BF16),
        *[pltpu.VMEM(block, BF16)] * 4,
        *[pltpu.VMEM(spectrum, F32)] * 4, pltpu.VMEM(spectrum, BF16),
        pltpu.VMEM((3,) + block, BF16), pltpu.VMEM((3,) + block, BF16),
        *[pltpu.VMEM((nc,) + bands, BF16)] * 2, *[pltpu.VMEM(bands, BF16)] * 2,
        pltpu.VMEM((1, w), F32), pltpu.VMEM((n, 1, w), F32),
        dma, *[dma(((n + 2) // 4,))] * 3, dma, dma((n // 2,)), dma, dma, pltpu.SemaphoreType.REGULAR,
        dma, dma((3,)), *[dma] * 6,
    ]
    operands = (*args[:8], skip.reshape(1, chan_width), forward, inverse)
    hbm, vmem = (pl.BlockSpec(memory_space=m) for m in (pltpu.HBM, pltpu.VMEM))
    outs = pl.pallas_call(
        functools.partial(kernel, n, nc, scale),
        out_shape=results,
        in_specs=[hbm] * 11,
        out_specs=(vmem,) * 6,
        scratch_shapes=scratch,
        compiler_params=pltpu.CompilerParams(
            collective_id=0, has_side_effects=True, vmem_limit_bytes=KERNEL_VMEM
        ),
    )(*[pltpu.with_memory_space_constraint(a, pltpu.HBM) for a in operands])
    outs = pl.pallas_call(
        store_all,
        out_shape=tuple(jax.ShapeDtypeStruct(o.shape, o.dtype) for o in outs),
        in_specs=[vmem] * 6,
        out_specs=(hbm,) * 6,
        scratch_shapes=[dma((6,))],
        compiler_params=pltpu.CompilerParams(vmem_limit_bytes=KERNEL_VMEM),
    )(*outs)
    return tuple(outs[:5]) + (outs[5].reshape(chan_width),)


def routed(*args):
    n, nc = lax.axis_size("seq"), lax.axis_size("chan")
    rows, chan_width = args[0].shape
    filter_width = args[7].shape[1]
    fits = chan_width % (n * LANES) == 0 and rows % (16 * nc) == 0 and rows % 32 == 0
    fits = fits and n % nc == 0 and n > 1 and n & (n - 1) == 0 and nc <= REACH + 2
    if fits and filter_width * nc == chan_width and filter_width % (chan_width // n) == 0:
        return fused_device(n, nc, *args)
    return per_device(*args)


def solution(mesh):
    return jax.shard_map(
        routed,
        mesh=mesh,
        in_specs=(
            P("seq", "chan"),
            P("seq", "chan"),
            P("seq", "chan"),
            P("seq", "chan"),
            P("seq", "chan"),
            P("seq", "chan"),
            P("seq", "chan"),
            P("seq", "chan"),
            P("chan"),
        ),
        out_specs=(
            P("seq", "chan"),
            P("seq", "chan"),
            P("seq", "chan"),
            P("seq", "chan"),
            P("seq", "chan"),
            P("chan"),
        ),
        check_vma=False,
    )
```

```python
import functools
import math

import jax
import jax.numpy as jnp
import numpy as np
from jax import lax
from jax.experimental import pallas as pl
from jax.experimental.pallas import tpu as pltpu
from jax.sharding import PartitionSpec as P

HIGHEST = lax.Precision.HIGHEST
LANES = 128
MESH = pl.DeviceIdType.MESH
BF16 = jnp.bfloat16
F32 = jnp.float32
KERNEL_VMEM = 32 * 2**20


def index_ramp(total):
    return jnp.arange(total, dtype=jnp.int32)


def widened(values):
    return values.astype(jnp.float32)


def angles(out_index, in_index, period, sign):
    phase_steps = out_index[:, None] * in_index[None, :] % period
    phase = phase_steps.astype(jnp.float32) * (sign * 2.0 * math.pi / period)
    return (jnp.cos(phase), jnp.sin(phase))


def times_table(left, right):
    return (left[0] * right[0] - left[1] * right[1], left[0] * right[1] + left[1] * right[0])


def block_table(pair):
    cosine, sine_part = pair
    return jnp.stack([jnp.stack([cosine, -sine_part]), jnp.stack([sine_part, cosine])])


def product_of(left, right):
    return jnp.stack(
        [left[0] * right[0] - left[1] * right[1], left[0] * right[1] + left[1] * right[0]]
    )


def conj_product(left, right):
    return jnp.stack(
        [left[0] * right[0] + left[1] * right[1], left[0] * right[1] - left[1] * right[0]]
    )


def joined(left, right):
    return jnp.concatenate([left, right], axis=-1)


def factor(total):
    chosen = 1
    for candidate in range(1, total + 1):
        if candidate * candidate <= total and total % candidate == 0:
            chosen = candidate
    return chosen


def leading_section(values, seq_size):
    cosine, sine_part = angles(index_ramp(2 * seq_size), index_ramp(seq_size), 2 * seq_size, -1.0)
    table = jnp.stack([cosine, sine_part])
    return jnp.einsum("rkp,pmc->rkmc", table, values, precision=HIGHEST)


def trailing_section(values, seq_size, period):
    cosine, sine_part = angles(index_ramp(seq_size), index_ramp(2 * seq_size), 2 * seq_size, 1.0)
    table = jnp.stack([cosine, -sine_part]) * (1.0 / period)
    return jnp.einsum("rpk,rkmc->pmc", table, values, precision=HIGHEST)


def inner_forward(values, freq_keys, period):
    lead_size, row_count, chan_count = values.shape[1:]
    outer_size = factor(row_count)
    inner_size = row_count // outer_size
    values = values.reshape(2, lead_size, outer_size, inner_size, chan_count)
    first_twiddle = angles(freq_keys, index_ramp(row_count), period, -1.0)
    first_twiddle = tuple(
        (part.reshape(lead_size, outer_size, inner_size) for part in first_twiddle)
    )
    outer_dft = angles(index_ramp(outer_size), index_ramp(outer_size), outer_size, -1.0)
    outer_table = times_table(
        tuple((part[None, :, :, None] for part in outer_dft)),
        tuple((part[:, None, :, :] for part in first_twiddle)),
    )
    values = jnp.einsum("rsjxab,sjabc->rjxbc", block_table(outer_table), values, precision=HIGHEST)
    second_twiddle = angles(index_ramp(outer_size), index_ramp(inner_size), row_count, -1.0)
    inner_dft = angles(index_ramp(inner_size), index_ramp(inner_size), inner_size, -1.0)
    inner_table = times_table(
        tuple((part[None, :, :] for part in inner_dft)),
        tuple((part[:, None, :] for part in second_twiddle)),
    )
    return jnp.einsum("rsxyb,sjxbc->rjxyc", block_table(inner_table), values, precision=HIGHEST)


def inner_inverse(values, freq_keys, period):
    lead_size, outer_size, inner_size, chan_count = values.shape[1:]
    row_count = outer_size * inner_size
    second_twiddle = angles(index_ramp(outer_size), index_ramp(inner_size), row_count, 1.0)
    inner_dft = angles(index_ramp(inner_size), index_ramp(inner_size), inner_size, 1.0)
    inner_table = times_table(
        tuple((part[:, :, None] for part in second_twiddle)),
        tuple((part[None, :, :] for part in inner_dft)),
    )
    values = jnp.einsum("rsxby,sjxyc->rjxbc", block_table(inner_table), values, precision=HIGHEST)
    first_twiddle = angles(freq_keys, index_ramp(row_count), period, 1.0)
    first_twiddle = tuple(
        (part.reshape(lead_size, outer_size, inner_size) for part in first_twiddle)
    )
    outer_dft = angles(index_ramp(outer_size), index_ramp(outer_size), outer_size, 1.0)
    outer_table = times_table(
        tuple((part[:, :, :, None] for part in first_twiddle)),
        tuple((part[None, :, None, :] for part in outer_dft)),
    )
    values = jnp.einsum("rsjabx,sjxbc->rjabc", block_table(outer_table), values, precision=HIGHEST)
    return values.reshape(2, lead_size, row_count, chan_count)


def forward_local(signal_part, seq_size):
    seq_length, chan_count = signal_part.shape
    row_count = seq_length // seq_size
    values = leading_section(signal_part.reshape(seq_size, row_count, chan_count), seq_size)
    return inner_forward(values, index_ramp(2 * seq_size), 2 * seq_length)


def inverse_local(values, seq_size):
    lead_size, outer_size, inner_size, chan_count = values.shape[1:]
    row_count = outer_size * inner_size
    period = 2 * seq_size * row_count
    values = inner_inverse(values, index_ramp(2 * seq_size), period)
    return trailing_section(values, seq_size, period).reshape(seq_size * row_count, chan_count)


def filter_times_pair(spec_filter, spec_pair):
    shape_pair = spec_pair.shape
    width = spec_filter.shape[-1]
    pair_view = spec_pair.reshape(shape_pair[:-1] + (2, width))
    filter_view = spec_filter[..., None, :]
    return product_of(filter_view, pair_view).reshape(shape_pair)


def per_device(fwd_q, fwd_k, fwd_v, bwd_q, bwd_k, bwd_v, bwd_grad, filters, skip):
    row_count, chan_width = fwd_q.shape
    seq_size = lax.axis_size("seq")
    grad_scale = 1.0 / math.sqrt(row_count * seq_size)
    source = (widened(fwd_k) * widened(fwd_v)).astype(jnp.bfloat16)
    second_source = (widened(bwd_k) * widened(bwd_v)).astype(jnp.bfloat16)
    upstream = (widened(bwd_grad) * widened(bwd_q)).astype(jnp.bfloat16)
    skip_gain = widened(skip)
    filters_all = lax.all_gather(filters, "chan", axis=1, tiled=True)
    narrow = chan_width // seq_size
    local_first, local_second = (
        lax.all_to_all(source, "seq", split_axis=1, concat_axis=0, tiled=True),
        lax.all_to_all(second_source, "seq", split_axis=1, concat_axis=0, tiled=True),
    )
    local_filter = lax.all_to_all(filters_all, "seq", split_axis=1, concat_axis=0, tiled=True)
    local_up = lax.all_to_all(upstream, "seq", split_axis=1, concat_axis=0, tiled=True)
    spec_sources = forward_local(
        widened(jnp.concatenate([local_first, local_second], axis=1)), seq_size
    )
    spec_filter = forward_local(local_filter, seq_size)
    conv_local = inverse_local(filter_times_pair(spec_filter, spec_sources), seq_size)
    conv_first, conv_second = (
        lax.all_to_all(conv_local[:, :narrow], "seq", split_axis=0, concat_axis=1, tiled=True),
        lax.all_to_all(conv_local[:, narrow:], "seq", split_axis=0, concat_axis=1, tiled=True),
    )
    spec_up = forward_local(widened(local_up), seq_size)
    spec_second = spec_sources[..., narrow:]
    back_local = inverse_local(
        joined(conj_product(spec_filter, spec_up), conj_product(spec_second, spec_up)), seq_size
    )
    through_conv, filter_terms = (
        lax.all_to_all(back_local[:, :narrow], "seq", split_axis=0, concat_axis=1, tiled=True),
        lax.all_to_all(
            back_local[:, narrow:] * grad_scale, "seq", split_axis=0, concat_axis=1, tiled=True
        ),
    )
    grad_filter = lax.psum_scatter(filter_terms, "chan", scatter_dimension=1, tiled=True)
    source_wide = widened(source)
    second_wide = widened(second_source)
    upstream_wide = widened(upstream)
    mixed = conv_first + skip_gain * source_wide
    output = (widened(fwd_q) * mixed).astype(jnp.bfloat16)
    mixed_two = conv_second + skip_gain * second_wide
    grad_query = (widened(bwd_grad) * mixed_two).astype(jnp.bfloat16)
    through = through_conv + skip_gain * upstream_wide
    grad_key = (through * widened(bwd_v)).astype(jnp.bfloat16)
    grad_value = (through * widened(bwd_k)).astype(jnp.bfloat16)
    grad_skip = lax.psum(jnp.sum(upstream_wide * second_wide, axis=0) * grad_scale, "seq")
    return (output, grad_query, grad_key, grad_value, grad_filter, grad_skip)


def block_tables(rows):
    freq = 2 * np.arange(rows)[:, None] + 1
    phase = (freq * np.arange(rows)[None, :] % (4 * rows)) * (np.pi / (2 * rows))
    forward = np.concatenate([np.cos(phase), -np.sin(phase)], axis=0)
    inverse = np.concatenate([np.cos(phase), -np.sin(phase)], axis=0).T / rows
    return forward.astype(np.float32), inverse.astype(np.float32)


REACH = 2


def kernel(
    n, nc, scale,
    fq_h, fk_h, fv_h, bq_h, bk_h, bv_h, bg_h, filt_h, skip_h, fwd_h, inv_h,
    out_o, gq_o, gk_o, gv_o, gf_o, gs_o,
    fq, fk, fv, bq, bk, bv, bg, filt, skip, fwd_t, inv_t, in_sem,
    s2_send, up_send, s1_send, f_send, fz, s2, up, s1, rf, spec_s, spec_u, spec_f, spec_w, prod,
    c_send, c_recv, g_send, zg, g2_send, g2_recv, k_send, k_recv,
    in_ss, s2_rs, up_rs, s1_rs, f_ss, f_rs, z_ss, z_rs, credit, c_ss, c_rs,
    gz_ss, gz_rs, g2_ss, g2_rs, k_ss, k_rs,
):
    rows, chan_width = fq.shape
    w = chan_width // n
    per = filt.shape[1] // w
    part, unit = rows // nc, w // nc
    me = lax.axis_index("seq")
    mz = lax.axis_index("chan")

    def flipped(r):
        at, bit = me, 1
        while bit < n:
            if r & bit:
                at = at + bit * (1 - 2 * lax.rem(me // bit, 2))
            bit *= 2
        return at

    order = sorted(range(1, n), key=lambda r: (r & 1, -r))
    peers = [flipped(r) for r in order]
    paired = list(zip(order, peers))
    upward = 2 * mz < nc
    zorder = []
    for k in range(nc - 1):
        j = nc - 1 - k
        zorder.append(jnp.where(upward, jnp.where(mz <= k, k + 1, k), jnp.where(mz >= j, j - 1, j)))

    def near(z):
        return (z - mz <= REACH) & (mz - z <= REACH)

    slot = lax.broadcasted_iota(jnp.int32, (part, w), 1) // unit
    own_slot = lax.rem(slot + nc - lax.rem(me, nc), nc)

    def turned(x, k):
        return pltpu.roll(x, (k % nc) * unit, 1) if k % nc else x

    def pick(choices, shift=None):
        out = choices[0]
        for k in range(1, nc):
            at = own_slot == k if shift is None else slot == (k + shift) % nc
            out = jnp.where(at, choices[k], out)
        return out

    def copy(src, dst, ss, rs, to):
        return pltpu.make_async_remote_copy(
            src_ref=src, dst_ref=dst, send_sem=ss, recv_sem=rs, device_id=to, device_id_type=MESH
        )

    def send(src, dst, ss, rs, to):
        copy(src, dst, ss, rs, to).start()

    def arrived(buf, rs):
        copy(buf, buf, rs, rs, {"seq": peers[0]}).wait_recv()

    def sent(buf, ss):
        copy(buf, buf, ss, ss, {"seq": peers[0]}).wait_send()

    span, count = 2 * rows, n // 2
    parts = [list(range(count))[i:i + 2] for i in range(0, count, 2)]

    def side(r):
        return len(parts) - 1 - (count - 1 - r // 2) // 2

    loads = (
        ((bk_h, bk), (bv_h, bv)), ((filt_h, filt),), ((bg_h, bg), (bq_h, bq)), ((fk_h, fk), (fv_h, fv), (fq_h, fq)),
        ((fwd_h, fwd_t),), ((inv_h, inv_t),), ((skip_h, skip),),
    )
    for at, group in enumerate(loads):
        for far, dst in group:
            pltpu.make_async_copy(far, dst, in_sem.at[at]).start()

    def loaded(*which):
        for at in which:
            whole = loads[at][0][1] if len(loads[at]) == 1 else c_send.at[pl.ds(0, len(loads[at]))]
            pltpu.make_async_copy(whole, whole, in_sem.at[at]).wait()

    barrier = pltpu.get_barrier_semaphore()
    for p in peers:
        pl.semaphore_signal(barrier, inc=1, device_id={"seq": p}, device_id_type=MESH)
    greeted = n - 1
    for z in zorder:
        greeted = greeted + near(z).astype(jnp.int32)

        @pl.when(near(z))
        def _(z=z):
            pl.semaphore_signal(barrier, inc=1, device_id={"chan": z}, device_id_type=MESH)

    chips = [flipped(r) // 2 for r in range(n - 2, 0, -2)] + [me // 2]

    def transform(dst, group, src):
        blocks = [jnp.concatenate([src[2 * c], src[2 * c + 1]], axis=0) for c in group]
        value = jnp.dot(fwd_t[...], jnp.concatenate(blocks, axis=1), preferred_element_type=F32)
        for i, c in enumerate(group):
            dst[c] = value[:, i * w:(i + 1) * w]

    def gated(dst, left, right):
        for k in range(nc):
            band_rows = slice(k * part, (k + 1) * part)
            for hi in range(per):
                pieces = []
                for o in range(nc):
                    cols = slice((o * per + hi) * w, (o * per + hi + 1) * w)
                    value = left[band_rows, cols].astype(F32) * right[band_rows, cols].astype(F32)
                    pieces.append(turned(value, o))
                for j in range(nc):
                    dst[hi * nc + j, band_rows] = pick(pieces, j).astype(BF16)

    loaded(0)
    gated(s2_send, bk, bv)
    loaded(1)
    for hi in range(per):
        cols = slice(hi * w, (hi + 1) * w)
        pieces = [turned(filt[k * part:(k + 1) * part, cols], k) for k in range(nc)]
        for j in range(nc):
            f_send[hi * nc + j] = pick(pieces, j).astype(BF16)
    pl.semaphore_wait(barrier, greeted)

    for r, p in paired:
        send(f_send.at[p], fz.at[mz, me], f_ss, f_rs.at[r // 2], {"seq": p})
    fz[mz, me] = f_send[me]

    distant = ~near(zorder[-1]) if nc > 1 else None
    if nc > 1:
        o = zorder[-1]
        other = jnp.where(o > mz, mz - 1, mz + 1)
        vouch = ((o - mz == REACH) | (mz - o == REACH)) & (other >= 0) & (other < nc)

        @pl.when(vouch)
        def _():
            pl.semaphore_signal(credit, inc=1, device_id={"chan": o}, device_id_type=MESH)

    def scatter(src, dst, ss, rs):
        for r, p in paired:
            send(src.at[p], dst.at[me], ss, rs.at[side(r)], {"seq": p})
        dst[me] = src[me]

    scatter(s2_send, s2, in_ss, s2_rs)
    loaded(2)
    gated(up_send, bg, bq)
    scatter(up_send, up, in_ss, up_rs)
    loaded(3)
    gated(s1_send, fk, fv)

    for i, c in enumerate(chips[::-1]):
        fresh = fz.at[mz, pl.ds(2 * c, 2)]
        arrived(fresh if i else fz.at[mz, pl.ds(0, 1)], f_rs.at[i])
        if nc > 1 and i == 0:
            @pl.when(distant)
            def _():
                pl.semaphore_wait(credit, 1)
        for k in range(nc - 2, -1, -1):
            send(fresh, fresh, z_ss, z_rs, {"chan": zorder[k]})
    loaded(4, 5)

    sign = 1.0 - 2.0 * lax.rem(lax.broadcasted_iota(jnp.int32, (16, w), 0), 2).astype(F32)

    def products(win, src, corr, raw=None):
        def tile(k, carry):
            re_at = pl.ds(pl.multiple_of(k * 16, 16), 16)
            im_at = pl.ds(pl.multiple_of(span + k * 16, 16), 16)
            if raw is None:
                ar = [win[d, re_at] for d in range(count)]
                ai = [win[d, im_at] for d in range(count)]
            else:
                br = [raw[d, re_at] for d in range(count)]
                bi = [raw[d, im_at] for d in range(count)]
                ar = br[:1] + [br[d] - sign * bi[d - 1] for d in range(1, count)]
                ai = bi[:1] + [bi[d] + sign * br[d - 1] for d in range(1, count)]
                for d in range(count if win is not None else 0):
                    win[d, re_at] = ar[d]
                    win[d, im_at] = ai[d]
            xr = [src[d, re_at] for d in range(count)]
            xi = [src[d, im_at] for d in range(count)]
            for b in range(count):
                terms = [(c - b, c) for c in range(b, count)] if corr else [(b - c, c) for c in range(b + 1)]
                re, im = None, None
                for d, c in terms:
                    if corr:
                        tr = ar[d] * xr[c] + ai[d] * xi[c]
                        ti = ar[d] * xi[c] - ai[d] * xr[c]
                    else:
                        tr = ar[d] * xr[c] - ai[d] * xi[c]
                        ti = ar[d] * xi[c] + ai[d] * xr[c]
                    re = tr if re is None else re + tr
                    im = ti if im is None else im + ti
                prod[b, re_at] = re.astype(BF16)
                prod[b, im_at] = im.astype(BF16)
            return carry

        lax.fori_loop(0, span // 16, tile, 0)

    def inverse(group):
        blocks = [prod[c] for c in group]
        value = jnp.dot(inv_t[...], jnp.concatenate(blocks, axis=1), preferred_element_type=F32)
        return [value[:, i * w:(i + 1) * w] for i in range(len(group))]

    def give_back(which, group):
        for r in group:
            p = flipped(r)
            send(c_send.at[which, p], c_recv.at[which, me], c_ss, c_rs.at[which], {"seq": p})

    def halves(dst, c, value):
        dst[2 * c] = value[:rows].astype(BF16)
        dst[2 * c + 1] = value[rows:].astype(BF16)


    def outputs(which, now):
        values = [inverse([chips[i] for i in group]) for group in parts]
        for group, results in zip(parts, values):
            for i, value in zip(group, results):
                halves(c_send.at[which], chips[i], value)
            if now:
                give_back(which, [r for i in group for r in (n - 2 - 2 * i, n - 1 - 2 * i) if r])
        c_recv[which, me] = c_send[which, me]

    def gather(buf, sems, spec):
        for at, group in enumerate(parts[::-1]):
            arrived(buf.at[pl.ds(0, 2 * len(group) - (at == 0))], sems.at[at])
            transform(spec, [chips[i] for i in group], buf)

    gather(s2, s2_rs, spec_s)
    scatter(s1_send, s1, in_ss, s1_rs)
    gather(up, up_rs, spec_u)
    products(None, spec_u, True, spec_s)
    for group in parts:
        for b, value in zip(group, inverse(group)):
            for h in range(2):
                bands = [(value[h * rows + k * part:h * rows + (k + 1) * part] * scale).astype(BF16) for k in range(nc)]
                for o in range(nc):
                    g_send[o, 2 * b + h] = pick([turned(bands[k], k - o) for k in range(nc)])

    for k in range(nc - 2, -1, -1):
        z = zorder[k]
        send(g_send.at[z], zg.at[jnp.where(mz > z, mz - 1, mz)], gz_ss, gz_rs, {"chan": z})

    if nc > 1:
        arrived(fz.at[pl.ds(0, nc - 1)], z_rs)
    for q in range(n):
        pieces = [fz[o, q] for o in range(nc)]
        for k in range(nc):
            rf[q, k * part:(k + 1) * part] = pick([turned(pieces[o], o - k) for o in range(nc)])
    for group in parts:
        transform(spec_f, group, rf)
    products(spec_w, spec_s, False, spec_f)
    outputs(0, True)

    products(spec_w, spec_u, True)
    outputs(1, True)

    total = jnp.zeros((1, w), F32)
    for q in range(n):
        total += jnp.sum(s2[q].astype(F32) * up[q].astype(F32), axis=0, keepdims=True)
    k_send[...] = total * scale
    for p in peers:
        send(k_send, k_recv.at[me], k_ss, k_rs, {"seq": p})
    k_recv[me] = k_send[...]

    gather(s1, s1_rs, spec_s)
    products(spec_w, spec_s, False)
    outputs(2, True)

    if nc > 1:
        arrived(zg.at[pl.ds(0, nc - 1)], gz_rs)
    for p in range(n):
        acc = g_send[mz, p].astype(F32)
        for k in range(nc - 1):
            acc += zg[k, p].astype(F32)
        g2_send[p] = acc.astype(BF16)
    for p in peers:
        send(g2_send.at[p], g2_recv.at[me], g2_ss, g2_rs, {"seq": p})
    g2_recv[me] = g2_send[me]

    loaded(6)

    def returned(which):
        arrived(c_recv.at[which, pl.ds(0, n - 1)], c_rs.at[which])
        for k in range(nc):
            at = slice(k * part, (k + 1) * part)
            for hi in range(per):
                values = [c_recv[which, hi * nc + j, at].astype(F32) for j in range(nc)]
                for o in range(nc):
                    cols = slice((o * per + hi) * w, (o * per + hi + 1) * w)
                    yield (at, cols), skip[:, cols], turned(pick(values, o), -o)

    def product(left, right, at):
        return (left[at].astype(F32) * right[at].astype(F32)).astype(BF16).astype(F32)

    for at, gain, value in returned(0):
        mixed = value + gain * product(bk, bv, at)
        gq_o[at] = (bg[at].astype(F32) * mixed).astype(BF16)
    arrived(k_recv.at[pl.ds(0, n - 1)], k_rs)
    sums = k_recv[...]
    for hi in range(per):
        for o in range(nc):
            cols = slice((o * per + hi) * w, (o * per + hi + 1) * w)
            value = sums[hi * nc]
            for j in range(1, nc):
                value = jnp.where(slot[:1] == (o + j) % nc, sums[hi * nc + j], value)
            gs_o[:, cols] = turned(value, -o)
    for at, gain, value in returned(1):
        through = value + gain * product(bg, bq, at)
        gk_o[at] = (through * bv[at].astype(F32)).astype(BF16)
        gv_o[at] = (through * bk[at].astype(F32)).astype(BF16)
    for at, gain, value in returned(2):
        mixed = value + gain * product(fk, fv, at)
        out_o[at] = (fq[at].astype(F32) * mixed).astype(BF16)

    arrived(g2_recv.at[pl.ds(0, n - 1)], g2_rs)
    for k in range(nc):
        for hi in range(per):
            value = pick([g2_recv[hi * nc + j].astype(F32) for j in range(nc)], k)
            gf_o[k * part:(k + 1) * part, hi * w:(hi + 1) * w] = turned(value, -k)

    sent(c_send.at[:, pl.ds(0, n - 1)], in_ss)
    sent(c_send.at[:, pl.ds(0, n - 1)], c_ss)
    sent(f_send.at[pl.ds(0, n - 1)], f_ss)
    sent(g2_send.at[pl.ds(0, n - 1)], g2_ss)
    sent(k_recv.at[pl.ds(0, n - 1)], k_ss)
    if nc > 1:
        sent(fz.at[pl.ds(0, nc - 1)], z_ss)
        sent(zg.at[pl.ds(0, nc - 1)], gz_ss)


def store_all(*refs):
    count = len(refs) // 2
    near, far, sems = refs[:count], refs[count:2 * count], refs[-1]
    stores = [pltpu.make_async_copy(near[i], far[i], sems.at[i]) for i in range(count)]
    for c in stores:
        c.start()
    for c in stores:
        c.wait()


def fused_device(n, nc, *args):
    fwd_q, filters, skip = args[0], args[7], args[8]
    rows, chan_width = fwd_q.shape
    w = chan_width // n
    per = filters.shape[1] // w
    part = rows // nc
    scale = 1.0 / math.sqrt(rows * n)
    forward, inverse = (jnp.asarray(t, dtype=BF16) for t in block_tables(2 * rows))
    results = (
        *[pltpu.VMEM((rows, chan_width), BF16)] * 4, pltpu.VMEM(filters.shape, F32), pltpu.VMEM((1, chan_width), F32),
    )
    dma = pltpu.SemaphoreType.DMA
    block, bands = (n, rows, w), (n, part, w)
    spectrum = (n // 2, 4 * rows, w)
    scratch = [
        *[pltpu.VMEM((rows, chan_width), BF16)] * 7, pltpu.VMEM(filters.shape, F32),
        pltpu.VMEM((1, chan_width), F32), pltpu.VMEM(forward.shape, BF16), pltpu.VMEM(inverse.shape, BF16),
        dma((7,)),
        *[pltpu.VMEM(block, BF16)] * 3, pltpu.VMEM(bands, BF16), pltpu.VMEM((nc,) + bands, BF16),
        *[pltpu.VMEM(block, BF16)] * 4,
        *[pltpu.VMEM(spectrum, F32)] * 4, pltpu.VMEM(spectrum, BF16),
        pltpu.VMEM((3,) + block, BF16), pltpu.VMEM((3,) + block, BF16),
        *[pltpu.VMEM((nc,) + bands, BF16)] * 2, *[pltpu.VMEM(bands, BF16)] * 2,
        pltpu.VMEM((1, w), F32), pltpu.VMEM((n, 1, w), F32),
        dma, *[dma(((n + 2) // 4,))] * 3, dma, dma((n // 2,)), dma, dma, pltpu.SemaphoreType.REGULAR,
        dma, dma((3,)), *[dma] * 6,
    ]
    operands = (*args[:8], skip.reshape(1, chan_width), forward, inverse)
    hbm, vmem = (pl.BlockSpec(memory_space=m) for m in (pltpu.HBM, pltpu.VMEM))
    outs = pl.pallas_call(
        functools.partial(kernel, n, nc, scale),
        out_shape=results,
        in_specs=[hbm] * 11,
        out_specs=(vmem,) * 6,
        scratch_shapes=scratch,
        compiler_params=pltpu.CompilerParams(
            collective_id=0, has_side_effects=True, vmem_limit_bytes=KERNEL_VMEM
        ),
    )(*[pltpu.with_memory_space_constraint(a, pltpu.HBM) for a in operands])
    outs = pl.pallas_call(
        store_all,
        out_shape=tuple(jax.ShapeDtypeStruct(o.shape, o.dtype) for o in outs),
        in_specs=[vmem] * 6,
        out_specs=(hbm,) * 6,
        scratch_shapes=[dma((6,))],
        compiler_params=pltpu.CompilerParams(vmem_limit_bytes=KERNEL_VMEM),
    )(*outs)
    return tuple(outs[:5]) + (outs[5].reshape(chan_width),)


def routed(*args):
    n, nc = lax.axis_size("seq"), lax.axis_size("chan")
    rows, chan_width = args[0].shape
    filter_width = args[7].shape[1]
    fits = chan_width % (n * LANES) == 0 and rows % (16 * nc) == 0 and rows % 32 == 0
    fits = fits and n % nc == 0 and n > 1 and n & (n - 1) == 0 and nc <= REACH + 2
    if fits and filter_width * nc == chan_width and filter_width % (chan_width // n) == 0:
        return fused_device(n, nc, *args)
    return per_device(*args)


def solution(mesh):
    return jax.shard_map(
        routed,
        mesh=mesh,
        in_specs=(
            P("seq", "chan"),
            P("seq", "chan"),
            P("seq", "chan"),
            P("seq", "chan"),
            P("seq", "chan"),
            P("seq", "chan"),
            P("seq", "chan"),
            P("seq", "chan"),
            P("chan"),
        ),
        out_specs=(
            P("seq", "chan"),
            P("seq", "chan"),
            P("seq", "chan"),
            P("seq", "chan"),
            P("seq", "chan"),
            P("chan"),
        ),
        check_vma=False,
    )
```
